32 devices in a mesh: rows: 8 (over y, x, core), grp: 4 (over z).
Axes of the slice: x: 2, y: 2, z: 4, core: 2. Of those that a mesh axis runs over, the one named last changes fastest.
Arguments:
- pivot_columns: bfloat16 [32, 10240, 256], P('rows', 'grp'), may hold values from -6 to 6
- previous: bfloat16 [32, 10240, 512], P('rows', 'grp'), may hold values from -0.59765625 to 0.59765625
- pivots: int32 [256], replicated, may hold values from 0 to 327679, as said below
- pivot_inverse: bfloat16 [256, 256], replicated, may hold values from -0.4 to 1.5
- orbitals: bfloat16 [10240, 1024], P('grp'), may hold values from -0.0625 to 0.0625
- slab_orbitals: bfloat16 [32, 1024], replicated, may hold values from -1 to 1
Outputs:
- new_vectors: bfloat16 [32, 10240, 256], P('rows', 'grp')
- mo_block: bfloat16 [256, 1024, 1024], P('rows', None, 'grp')
The draws below stay inside these ranges and needn't reach their ends.
Inputs may be any that keep to these rules, and one draw needn't show every extreme that they name: `pivots`: distinct entries.
All inputs are finite; a program needn't handle non-finite values.
Results may differ from the reference program's by a relative error of at most 0.0038.
The reference program's roundings to bfloat16 on the way (of `pivot_rows`, `residual_columns`, `upper` and `half`) count: a program that leaves them out, or rounds other values in their place, can miss the bound.
Values may be sent and summed in bfloat16 or wider, within the bound.
A program may use at most 128 MiB of HBM per device.

```python
import jax
import jax.numpy as jnp

NBAS = 10240
NOCC = 1024
K_PREV = 512
NP = 256
MU = 32


def draw_pivots(key, part):
    chosen = jax.random.permutation(key, MU * NBAS)[:NP]
    return chosen.astype(jnp.int32)


def draw_pivot_inverse(key, part):
    first, second = jax.random.split(jax.random.fold_in(key, 17))
    spread = jax.random.normal(first, (NP, NP), jnp.float32) * NP ** (-0.5)
    spread = jnp.clip(spread, -0.39, 0.39)
    diagonal = jax.random.uniform(second, (NP,), jnp.float32, 0.5, 1.5)
    eye_mask = jnp.arange(NP)[:, None] == jnp.arange(NP)[None, :]
    return jnp.where(eye_mask, diagonal[None, :], spread).astype(jnp.bfloat16)


def shard_levels(key, dims, cuts, low, largest):
    loudness = 1.0
    for position, blocks in cuts:
        heights = jax.random.uniform(jax.random.fold_in(jax.random.fold_in(key, 6), position), (blocks,), jnp.float32, low / len(cuts), largest / len(cuts))
        loudness = loudness * jnp.repeat(jnp.exp(heights), dims[position] // blocks).reshape((-1,) + (1,) * (len(dims) - 1 - position))
    return loudness


def scatter_about(rng, dims, deviation, reach, shards=(), dtype=jnp.bfloat16):
    entries = deviation * jax.random.normal(rng, dims, jnp.float32)
    if shards:
        entries = entries * shard_levels(rng, dims, shards, -0.22, 0.18)
    return jnp.clip(entries, -reach, reach).astype(dtype)


def setup_inputs(seed: int = 0) -> dict:
    arg_keys = jax.random.split(jax.random.key(seed), 7)
    return {
        "pivot_columns": scatter_about(arg_keys[0], (MU, NBAS, NP), 1.0, 6.0, ((0, 8), (1, 4))),
        "previous": scatter_about(arg_keys[1], (MU, NBAS, K_PREV), 0.1, 0.59765625, ((0, 8), (1, 4))),
        "pivots": draw_pivots(jax.random.fold_in(arg_keys[6], 71), 0),
        "pivot_inverse": draw_pivot_inverse(jax.random.fold_in(arg_keys[6], 71), 0),
        "orbitals": scatter_about(arg_keys[4], (NBAS, NOCC), NBAS ** -0.5, 0.0625, ((0, 4),)),
        "slab_orbitals": scatter_about(arg_keys[5], (MU, NOCC), MU ** -0.5, 1.0),
    }


def reference(pivot_columns, previous, pivots, pivot_inverse, orbitals, slab_orbitals):
    prev_count = previous.shape[2]
    flat_prev = previous.reshape(MU * NBAS, prev_count)
    pivot_rows = jnp.take(flat_prev, pivots.astype(jnp.int32), axis=0)
    correction = jnp.dot(flat_prev, pivot_rows.T, preferred_element_type=jnp.float32)
    flat_columns = pivot_columns.reshape(MU * NBAS, NP)
    residual_columns = (flat_columns.astype(jnp.float32) - correction).astype(jnp.bfloat16)
    upper = jnp.triu(pivot_inverse)
    new_flat = jnp.dot(residual_columns, upper, preferred_element_type=jnp.float32).astype(jnp.bfloat16)
    new_vectors = new_flat.reshape(MU, NBAS, NP)
    by_second = jnp.transpose(new_vectors, (1, 0, 2)).reshape(NBAS, MU * NP)
    half = jnp.dot(orbitals.T, by_second, preferred_element_type=jnp.float32).astype(jnp.bfloat16)
    half = half.reshape(NOCC, MU, NP)
    by_first = jnp.transpose(half, (1, 0, 2)).reshape(MU, NOCC * NP)
    full = jnp.dot(slab_orbitals.T, by_first, preferred_element_type=jnp.float32).astype(jnp.bfloat16)
    mo_block = jnp.transpose(full.reshape(NOCC, NOCC, NP), (2, 0, 1))
    return new_vectors, mo_block
```

```python
import functools

import jax
import jax.numpy as jnp
from jax import lax
from jax.experimental import pallas as pl
from jax.experimental.pallas import tpu as pltpu
from jax.sharding import PartitionSpec as P

F32 = jnp.float32
BF16 = jnp.bfloat16
MESH = pl.DeviceIdType.MESH


def chained(G):
    return G <= 4


def group_orders(G):
    def due(g, d):
        if d == g:
            return 4 * G
        return 2 * (G - 1 - d) + g if d > g else 2 * d + G - 1 - g

    return [sorted(range(G), key=lambda d: (due(g, d), d)) for g in range(G)]


def choose(g, values):
    chosen = jnp.int32(values[0])
    for k in range(1, len(values)):
        chosen = jnp.where(g == k, values[k], chosen)
    return chosen


def fused_kernel(
    R, G, piv_ref, pc_hbm, prev_hbm, inv_ref, orb_hbm, out_hbm, new_v,
    piv_col, picked, buf_x, buf_a, buf_b, buf_c, rows_v, upper_v, prev_v, orb_v, turned, block_v, send, in_up, in_down,
    send_a, recv_a, send_b, recv_b, send_c, recv_c, prev_sem, pc_sem, orb_sem,
    own_sem, hop_sem, up_sem, down_sem, send_sem, recv_sem,
):
    r = lax.axis_index("rows")
    g = lax.axis_index("grp")
    N = R * G
    me = r * G + g
    mu_dev, nu, p = new_v.shape
    _, _, _, pl_dev, j_dev = send.shape
    c = buf_c.shape[1]

    load_prev = [pltpu.make_async_copy(prev_hbm.at[mu], prev_v.at[mu], prev_sem.at[mu]) for mu in range(mu_dev)]
    load_orb = pltpu.make_async_copy(orb_hbm, orb_v, orb_sem)

    def load_pc(mu):
        return pltpu.make_async_copy(pc_hbm.at[mu], new_v.at[mu], pc_sem.at[mu])

    for copy in load_prev:
        copy.start()
    for mu in range(mu_dev):
        load_pc(mu).start()
    load_orb.start()

    barrier = pltpu.get_barrier_semaphore()

    @pl.loop(1, N)
    def _(d):
        peer = lax.rem(me + d, N)
        pl.semaphore_signal(
            barrier, inc=1, device_id={"rows": peer // G, "grp": lax.rem(peer, G)}, device_id_type=MESH
        )

    shape = (p, p)
    low = lax.broadcasted_iota(jnp.int32, shape, 0)
    high = lax.broadcasted_iota(jnp.int32, shape, 1)
    upper_v[...] = jnp.where(low <= high, inv_ref[...].astype(F32), 0.0).astype(BF16)

    lanes = piv_col.shape[1]
    piv_col[...] = jnp.broadcast_to(piv_ref[...], (lanes, p)).T
    picked[...] = jnp.zeros(picked.shape, F32)
    piece = 512 if nu % 512 == 0 else 256
    for mu in range(mu_dev):
        load_prev[mu].wait()
        base = (r * mu_dev + mu) * (nu * G) + g * nu

        @pl.loop(0, nu // piece)
        def _(i):
            start = pl.multiple_of(i * piece, piece)
            at = lax.broadcasted_iota(jnp.int32, (p, lanes), 1) + (base + start)
            hot = jnp.concatenate(
                [jnp.where(piv_col[...] == at + k * lanes, 1.0, 0.0).astype(BF16) for k in range(piece // lanes)], axis=1
            )
            picked[...] += jnp.dot(hot, prev_v[mu, pl.ds(start, piece), :], preferred_element_type=F32)

    for k in range(R):
        buf_x[k] = picked[k * c : (k + 1) * c, :].astype(BF16)
    pl.semaphore_wait(barrier, N - 1)

    def remote(src, dst, send, recv, row, grp):
        return pltpu.make_async_remote_copy(
            src_ref=src, dst_ref=dst, send_sem=send, recv_sem=recv,
            device_id={"rows": row, "grp": grp}, device_id_type=MESH,
        )

    row_peers = [(d, lax.rem(r + d, R)) for d in range(1, R)]
    grp_peers = [(d, lax.rem(g + d, G)) for d in range(1, G)]
    first = [remote(buf_x.at[q], buf_a.at[d], send_a.at[d], recv_a.at[d], q, g) for d, q in row_peers]
    for copy in first:
        copy.start()
    total = buf_x[r].astype(F32)
    for (d, _), copy in zip(row_peers, first):
        copy.wait_recv()
        total = total + buf_a[d].astype(F32)
    buf_b[0] = total.astype(BF16)
    second = [remote(buf_b.at[0], buf_b.at[d], send_b.at[d], recv_b.at[d], r, q) for d, q in grp_peers]
    for copy in second:
        copy.start()
    for (d, _), copy in zip(grp_peers, second):
        copy.wait_recv()
        total = total + buf_b[d].astype(F32)
    buf_c[r] = total.astype(BF16)
    third = [remote(buf_c.at[r], buf_c.at[r], send_c.at[d], recv_c.at[d], q, g) for d, q in row_peers]
    for copy in third:
        copy.start()
    for copy in third:
        copy.wait_recv()
    for copy in first + second + third:
        copy.wait_send()
    for k in range(R):
        picked[k * c : (k + 1) * c, :] = buf_c[k].astype(F32)
    rows_v[...] = picked[...].astype(BF16)
    load_orb.wait()

    chunk = 512 if nu % 512 == 0 else 256
    orders = group_orders(G)

    def make_vectors(mu):
        load_pc(mu).wait()
        eye = jnp.where(
            lax.broadcasted_iota(jnp.int32, shape, 0) == lax.broadcasted_iota(jnp.int32, shape, 1), 1.0, 0.0
        ).astype(BF16)

        @pl.loop(0, nu // chunk)
        def _(i):
            at = pl.ds(pl.multiple_of(i * chunk, chunk), chunk)
            correction = lax.dot_general(
                prev_v[mu, at, :], rows_v[...], (((1,), (1,)), ((), ())), preferred_element_type=F32
            )
            residual = (new_v[mu, at, :].astype(F32) - correction).astype(BF16)
            made = jnp.dot(residual, upper_v[...], preferred_element_type=F32).astype(BF16)
            new_v[mu, at, :] = made
            turned[mu, :, at] = lax.dot_general(
                eye, made, (((1,), (1,)), ((), ())), preferred_element_type=F32
            ).astype(BF16)

    def add(buf, slot, sem, mu):
        here = buf.at[slot, mu]
        pltpu.make_async_copy(here, here, sem.at[slot, mu]).wait()
        for k in range(R):
            block_v[k * pl_dev : (k + 1) * pl_dev, :] += buf[slot, mu, k].astype(F32)

    for s in range(G):
        to = choose(g, [order[s] for order in orders])
        own = s == G - 1

        @pl.loop(0, mu_dev)
        def _(mu):
            if s == 0:
                make_vectors(mu)
            cols = pl.ds(pl.multiple_of(to * j_dev, j_dev), j_dev)
            block_v[...] = jnp.dot(turned[mu], orb_v[:, cols], preferred_element_type=F32)
            if chained(G):
                if G > 1:
                    pl.when((to >= g) & (g > 0))(lambda: add(in_up, to, up_sem, mu))
                    pl.when((to <= g) & (g < G - 1))(lambda: add(in_down, to, down_sem, mu))
            elif own:
                for d, q in grp_peers:
                    add(in_up, q, up_sem, mu)
            for k in range(R):
                send[to, mu, k] = block_v[k * pl_dev : (k + 1) * pl_dev, :].astype(BF16)
            if own:
                for k in range(R):
                    peer = lax.rem(r + k, R)
                    src = send.at[to, mu, peer]
                    dst = out_hbm.at[r * mu_dev + mu]
                    if k:
                        remote(src, dst, send_sem, recv_sem, peer, g).start()
                    else:
                        pltpu.make_async_copy(src, dst, own_sem).start()
            elif chained(G):
                @pl.when(to > g)
                def _():
                    remote(send.at[to, mu], in_up.at[to, mu], hop_sem, up_sem.at[to, mu], r, g + 1).start()

                @pl.when(to < g)
                def _():
                    remote(send.at[to, mu], in_down.at[to, mu], hop_sem, down_sem.at[to, mu], r, g - 1).start()
            else:
                remote(send.at[to, mu], in_up.at[g, mu], hop_sem, up_sem.at[g, mu], r, to).start()

    own = out_hbm.at[pl.ds(0, mu_dev)]
    pltpu.make_async_copy(own, own, own_sem).wait()
    if G > 1:
        hops = send.at[pl.ds(0, G - 1)]
        pltpu.make_async_copy(hops, hops, hop_sem).wait()
    if R > 1:
        every = out_hbm.at[pl.ds(0, (R - 1) * mu_dev)]
        pltpu.make_async_copy(every, every, send_sem).wait()
        pltpu.make_async_copy(every, every, recv_sem).wait()


def fused(pivots, columns, previous, inverse, orbitals, R, G):
    mu_dev, nu, p = columns.shape
    k = previous.shape[2]
    c = p // R
    nj = orbitals.shape[1]
    hbm = pl.BlockSpec(memory_space=pl.ANY)
    vmem = pl.BlockSpec(memory_space=pltpu.VMEM)
    dma = pltpu.SemaphoreType.DMA
    return pl.pallas_call(
        functools.partial(fused_kernel, R, G),
        out_shape=(
            jax.ShapeDtypeStruct((R * mu_dev, c, nj // G), BF16),
            jax.ShapeDtypeStruct(columns.shape, BF16),
        ),
        in_specs=[vmem, hbm, hbm, vmem, hbm],
        out_specs=(hbm, vmem),
        scratch_shapes=[
            pltpu.VMEM((p, 128), jnp.int32),
            pltpu.VMEM((p, k), F32),
            pltpu.VMEM((R, c, k), BF16),
            pltpu.VMEM((R, c, k), BF16),
            pltpu.VMEM((G, c, k), BF16),
            pltpu.VMEM((R, c, k), BF16),
            pltpu.VMEM((p, k), BF16),
            pltpu.VMEM((p, p), BF16),
            pltpu.VMEM((mu_dev, nu, k), BF16),
            pltpu.VMEM((nu, nj), BF16),
            pltpu.VMEM((mu_dev, p, nu), BF16),
            pltpu.VMEM((p, nj // G), F32),
            pltpu.VMEM((G, mu_dev, R, c, nj // G), BF16),
            pltpu.VMEM((G, mu_dev, R, c, nj // G), BF16),
            pltpu.VMEM((G, mu_dev, R, c, nj // G), BF16),
            dma((R,)), dma((R,)), dma((G,)), dma((G,)), dma((R,)), dma((R,)),
            dma((mu_dev,)), dma((mu_dev,)), dma(()),
            dma(()), dma(()), dma((G, mu_dev)), dma((G, mu_dev)), dma(()), dma(()),
        ],
        compiler_params=pltpu.CompilerParams(
            collective_id=0, has_side_effects=True, vmem_limit_bytes=48 * 1024 * 1024
        ),
        name="fused_exchange",
    )(pivots, columns, previous, inverse, orbitals)


def block_kernel(part_ref, slab_ref, made_ref, out_ref, new_hbm, sorted_ref, slab_t_ref, new_sem):
    rows, _ = part_ref.shape
    mus = slab_ref.shape[0]
    block = out_ref.shape[0]
    vecs = rows // mus
    step = pl.program_id(0)
    store = pltpu.make_async_copy(made_ref, new_hbm, new_sem)

    @pl.when(step == 0)
    def _():
        store.start()
        slab_t_ref[...] = slab_ref[...].astype(F32).T.astype(BF16)
        piece = 128
        shift = mus.bit_length() - 1

        @pl.loop(0, rows // piece)
        def _(i):
            at = pl.ds(pl.multiple_of(i * piece, piece), piece)
            row = lax.broadcasted_iota(jnp.int32, (piece, rows), 0) + i * piece
            col = lax.broadcasted_iota(jnp.int32, (piece, rows), 1)
            source = (row & (mus - 1)) * vecs + lax.shift_right_logical(row, shift)
            pick = jnp.where(source == col, 1.0, 0.0).astype(BF16)
            sorted_ref[at, :] = jnp.dot(pick, part_ref[...], preferred_element_type=F32).astype(BF16)

    for q in range(block):
        at = pl.ds(pl.multiple_of((step * block + q) * mus, mus), mus)
        out_ref[q] = jnp.dot(slab_t_ref[...], sorted_ref[at, :], preferred_element_type=F32).astype(BF16)

    @pl.when(step == pl.num_programs(0) - 1)
    def _():
        store.wait()


def orbital_block(part, slab, made):
    rows, j = part.shape
    mus, i = slab.shape
    assert mus & (mus - 1) == 0
    vecs = rows // mus
    block = 4 if vecs % 4 == 0 else 1
    return pl.pallas_call(
        block_kernel,
        grid=(vecs // block,),
        out_shape=(
            jax.ShapeDtypeStruct((vecs, i, j), BF16),
            jax.ShapeDtypeStruct(made.shape, BF16),
        ),
        in_specs=[
            pl.BlockSpec((rows, j), lambda s: (0, 0)),
            pl.BlockSpec((mus, i), lambda s: (0, 0)),
            pl.BlockSpec(memory_space=pltpu.VMEM),
        ],
        out_specs=(pl.BlockSpec((block, i, j), lambda s: (s, 0, 0)), pl.BlockSpec(memory_space=pl.ANY)),
        scratch_shapes=[
            pltpu.VMEM((rows, j), BF16),
            pltpu.VMEM((i, mus), BF16),
            pltpu.SemaphoreType.DMA(()),
        ],
        compiler_params=pltpu.CompilerParams(vmem_limit_bytes=40 * 1024 * 1024),
        name="orbital_block",
    )(part, slab, made)


def per_device(R, G, pivot_columns, previous, pivots, pivot_inverse, orbitals, slab_orbitals):
    mu_dev = previous.shape[0]
    count = pivot_columns.shape[2]
    part, made = fused(
        pivots.reshape(1, count), pivot_columns, previous, pivot_inverse, orbitals, R, G
    )
    part = part.reshape(R * mu_dev * (count // R), orbitals.shape[1] // G)
    mo_block, new_vectors = orbital_block(part, slab_orbitals, made)
    return new_vectors, mo_block


def solution(mesh):
    R, G = mesh.shape["rows"], mesh.shape["grp"]
    in_specs = (P("rows", "grp", None), P("rows", "grp", None), P(), P(), P("grp", None), P())
    out_specs = (P("rows", "grp", None), P("rows", None, "grp"))
    return jax.shard_map(
        functools.partial(per_device, R, G), mesh=mesh, in_specs=in_specs, out_specs=out_specs,
        check_vma=False,
    )
```

```python
import functools

import jax
import jax.numpy as jnp
from jax import lax
from jax.experimental import pallas as pl
from jax.experimental.pallas import tpu as pltpu
from jax.sharding import PartitionSpec as P

F32 = jnp.float32
BF16 = jnp.bfloat16
MESH = pl.DeviceIdType.MESH


def chained(G):
    return G <= 4


def group_orders(G):
    def due(g, d):
        if d == g:
            return 4 * G
        return 2 * (G - 1 - d) + g if d > g else 2 * d + G - 1 - g

    return [sorted(range(G), key=lambda d: (due(g, d), d)) for g in range(G)]


def choose(g, values):
    chosen = jnp.int32(values[0])
    for k in range(1, len(values)):
        chosen = jnp.where(g == k, values[k], chosen)
    return chosen


def fused_kernel(
    R, G, piv_hbm, pc_hbm, prev_hbm, inv_hbm, orb_hbm, out_hbm, new_v,
    piv_v, inv_v, piv_col, hot_v, picked, buf_x, buf_a, buf_b, buf_c, rows_t, upper_v, prev_v, orb_v, orb_t,
    block_v, send, in_up, in_down, fin_v,
    send_a, recv_a, send_b, recv_b, send_c, recv_c, small_sem, prev_sem, pc_sem, orb_sem,
    own_sem, hop_sem, up_sem, down_sem, send_sem, recv_sem,
):
    r = lax.axis_index("rows")
    g = lax.axis_index("grp")
    N = R * G
    me = r * G + g
    mu_dev, nu, p = new_v.shape
    _, _, j_dev, _ = send.shape
    halves, _, c, kh = buf_c.shape

    load_piv = pltpu.make_async_copy(piv_hbm, piv_v, small_sem.at[0])
    load_inv = pltpu.make_async_copy(inv_hbm, inv_v, small_sem.at[1])
    load_orb = pltpu.make_async_copy(orb_hbm, orb_v, orb_sem)

    def load_prev(h, mu):
        at = pl.ds(h * kh, kh)
        return pltpu.make_async_copy(prev_hbm.at[mu, :, at], prev_v.at[mu, :, at], prev_sem.at[h, mu])

    def load_pc(mu):
        return pltpu.make_async_copy(pc_hbm.at[mu], new_v.at[mu], pc_sem.at[mu])

    load_piv.start()
    for h in range(halves):
        for mu in range(mu_dev):
            load_prev(h, mu).start()
    load_inv.start()

    barrier = pltpu.get_barrier_semaphore()

    @pl.loop(1, N)
    def _(d):
        peer = lax.rem(me + d, N)
        pl.semaphore_signal(
            barrier, inc=1, device_id={"rows": peer // G, "grp": lax.rem(peer, G)}, device_id_type=MESH
        )

    lanes = piv_col.shape[1]
    load_piv.wait()
    piv_col[...] = jnp.broadcast_to(piv_v[...], (lanes, p)).T
    for mu in range(mu_dev):
        base = (r * mu_dev + mu) * (nu * G) + g * nu

        @pl.loop(0, nu // lanes)
        def _(i):
            start = pl.multiple_of(i * lanes, lanes)
            at = lax.broadcasted_iota(jnp.int32, (p, lanes), 1) + (base + start)
            hot_v[mu, :, pl.ds(start, lanes)] = jnp.where(piv_col[...] == at, 1.0, 0.0).astype(BF16)

    def remote(src, dst, send, recv, row, grp):
        return pltpu.make_async_remote_copy(
            src_ref=src, dst_ref=dst, send_sem=send, recv_sem=recv,
            device_id={"rows": row, "grp": grp}, device_id_type=MESH,
        )

    row_peers = [(d, lax.rem(r + d, R)) for d in range(1, R)]
    grp_peers = [(d, lax.rem(g + d, G)) for d in range(1, G)]

    def pick(h):
        picked[...] = jnp.zeros(picked.shape, F32)

        @pl.loop(0, mu_dev)
        def _(mu):
            load_prev(h, mu).wait()
            picked[...] += jnp.dot(hot_v[mu], prev_v[mu, :, h * kh : (h + 1) * kh], preferred_element_type=F32)

        for k in range(R):
            buf_x[h, k] = picked[k * c : (k + 1) * c, :].astype(BF16)

    def first(h):
        return [
            remote(buf_x.at[h, q], buf_a.at[h, d], send_a.at[h, d], recv_a.at[h, d], q, g) for d, q in row_peers
        ]

    def second(h):
        return [
            remote(buf_b.at[h, 0], buf_b.at[h, d], send_b.at[h, d], recv_b.at[h, d], r, q) for d, q in grp_peers
        ]

    def third(h):
        return [
            remote(buf_c.at[h, r], buf_c.at[h, r], send_c.at[h, d], recv_c.at[h, d], q, g) for d, q in row_peers
        ]

    def add_rows(h):
        total = buf_x[h, r].astype(F32)
        for (d, _), copy in zip(row_peers, first(h)):
            copy.wait_recv()
            total = total + buf_a[h, d].astype(F32)
        buf_b[h, 0] = total.astype(BF16)
        for copy in second(h):
            copy.start()

    def add_groups(h):
        total = buf_b[h, 0].astype(F32)
        for (d, _), copy in zip(grp_peers, second(h)):
            copy.wait_recv()
            total = total + buf_b[h, d].astype(F32)
        buf_c[h, r] = total.astype(BF16)
        for copy in third(h):
            copy.start()

    def take_rows(h):
        for copy in third(h):
            copy.wait_recv()
        for k in range(R):
            picked[k * c : (k + 1) * c, :] = buf_c[h, k].astype(F32)
        rows_t[h * kh : (h + 1) * kh, :] = picked[...].T.astype(BF16)

    square = (256, 256)
    eye = jnp.where(
        lax.broadcasted_iota(jnp.int32, square, 0) == lax.broadcasted_iota(jnp.int32, square, 1), 1.0, 0.0
    ).astype(BF16)
    wide = orb_v.shape[1] // 256

    def turn_orbitals(first, last):
        @pl.loop(first, last)
        def _(i):
            at = pl.ds(pl.multiple_of(i * 256, 256), 256)
            for q in range(wide):
                orb_t[q * 256 : (q + 1) * 256, at] = lax.dot_general(
                    eye, orb_v[at, q * 256 : (q + 1) * 256], (((1,), (1,)), ((), ())), preferred_element_type=F32
                ).astype(BF16)

    tiles = nu // 256
    cuts = [tiles * k // (2 * halves) for k in range(2 * halves + 1)]
    for h in range(halves):
        pick(h)
        if h == 0:
            load_orb.start()
            for mu in range(mu_dev):
                load_pc(mu).start()
            pl.semaphore_wait(barrier, N - 1)
        for copy in first(h):
            copy.start()
    load_inv.wait()
    low = lax.broadcasted_iota(jnp.int32, (p, p), 0)
    high = lax.broadcasted_iota(jnp.int32, (p, p), 1)
    upper_v[...] = jnp.where(low <= high, inv_v[...].astype(F32), 0.0).astype(BF16)
    load_orb.wait()
    for h in range(halves):
        add_rows(h)
        turn_orbitals(cuts[h], cuts[h + 1])
    for h in range(halves):
        add_groups(h)
        turn_orbitals(cuts[halves + h], cuts[halves + h + 1])
    for h in range(halves):
        take_rows(h)

    chunk = 512 if nu % 512 == 0 else 256
    orders = group_orders(G)

    def make_vectors(mu):
        load_pc(mu).wait()
        for i in range(nu // chunk):
            at = pl.ds(i * chunk, chunk)
            correction = jnp.dot(prev_v[mu, at, :], rows_t[...], preferred_element_type=F32)
            residual = (new_v[mu, at, :].astype(F32) - correction).astype(BF16)
            new_v[mu, at, :] = jnp.dot(residual, upper_v[...], preferred_element_type=F32).astype(BF16)

    def add(buf, slot, sem, mu):
        here = buf.at[slot, mu]
        pltpu.make_async_copy(here, here, sem.at[slot, mu]).wait()
        block_v[...] += buf[slot, mu].astype(F32)

    for s in range(G):
        to = choose(g, [order[s] for order in orders])
        own = s == G - 1

        @pl.loop(0, mu_dev)
        def _(mu):
            if s == 0:
                make_vectors(mu)
            at = pl.ds(pl.multiple_of(to * j_dev, j_dev), j_dev)
            block_v[...] = jnp.dot(orb_t[at, :], new_v[mu], preferred_element_type=F32)
            if chained(G):
                if G > 1:
                    pl.when((to >= g) & (g > 0))(lambda: add(in_up, to, up_sem, mu))
                    pl.when((to <= g) & (g < G - 1))(lambda: add(in_down, to, down_sem, mu))
            elif own:
                for d, q in grp_peers:
                    add(in_up, q, up_sem, mu)
            if own:
                half = block_v[...].T.astype(BF16)
                for k in range(R):
                    fin_v[mu, k] = half[k * c : (k + 1) * c, :]
                for k in range(R):
                    peer = lax.rem(r + k, R)
                    src = fin_v.at[mu, peer]
                    dst = out_hbm.at[r * mu_dev + mu]
                    if k:
                        remote(src, dst, send_sem, recv_sem, peer, g).start()
                    else:
                        pltpu.make_async_copy(src, dst, own_sem).start()
                return
            send[to, mu] = block_v[...].astype(BF16)
            if chained(G):
                @pl.when(to > g)
                def _():
                    remote(send.at[to, mu], in_up.at[to, mu], hop_sem, up_sem.at[to, mu], r, g + 1).start()

                @pl.when(to < g)
                def _():
                    remote(send.at[to, mu], in_down.at[to, mu], hop_sem, down_sem.at[to, mu], r, g - 1).start()
            else:
                remote(send.at[to, mu], in_up.at[g, mu], hop_sem, up_sem.at[g, mu], r, to).start()

    for h in range(halves):
        for copy in first(h) + second(h) + third(h):
            copy.wait_send()
    own = out_hbm.at[pl.ds(0, mu_dev)]
    pltpu.make_async_copy(own, own, own_sem).wait()
    if G > 1:
        hops = send.at[pl.ds(0, G - 1)]
        pltpu.make_async_copy(hops, hops, hop_sem).wait()
    if R > 1:
        every = out_hbm.at[pl.ds(0, (R - 1) * mu_dev)]
        pltpu.make_async_copy(every, every, send_sem).wait()
        pltpu.make_async_copy(every, every, recv_sem).wait()


def fused(pivots, columns, previous, inverse, orbitals, R, G):
    mu_dev, nu, p = columns.shape
    k = previous.shape[2]
    c = p // R
    nj = orbitals.shape[1]
    halves = 2
    kh = k // halves
    hbm = pl.BlockSpec(memory_space=pltpu.HBM)
    anywhere = pl.BlockSpec(memory_space=pl.ANY)
    vmem = pl.BlockSpec(memory_space=pltpu.VMEM)
    dma = pltpu.SemaphoreType.DMA
    return pl.pallas_call(
        functools.partial(fused_kernel, R, G),
        out_shape=(
            jax.ShapeDtypeStruct((R * mu_dev, c, nj // G), BF16),
            jax.ShapeDtypeStruct(columns.shape, BF16),
        ),
        in_specs=[hbm, hbm, hbm, hbm, hbm],
        out_specs=(anywhere, vmem),
        scratch_shapes=[
            pltpu.VMEM((1, p), jnp.int32),
            pltpu.VMEM((p, p), BF16),
            pltpu.VMEM((p, 128), jnp.int32),
            pltpu.VMEM((mu_dev, p, nu), BF16),
            pltpu.VMEM((p, kh), F32),
            pltpu.VMEM((halves, R, c, kh), BF16),
            pltpu.VMEM((halves, R, c, kh), BF16),
            pltpu.VMEM((halves, G, c, kh), BF16),
            pltpu.VMEM((halves, R, c, kh), BF16),
            pltpu.VMEM((k, p), BF16),
            pltpu.VMEM((p, p), BF16),
            pltpu.VMEM((mu_dev, nu, k), BF16),
            pltpu.VMEM((nu, nj), BF16),
            pltpu.VMEM((nj, nu), BF16),
            pltpu.VMEM((nj // G, p), F32),
            pltpu.VMEM((G, mu_dev, nj // G, p), BF16),
            pltpu.VMEM((G, mu_dev, nj // G, p), BF16),
            pltpu.VMEM((G, mu_dev, nj // G, p), BF16),
            pltpu.VMEM((mu_dev, R, c, nj // G), BF16),
            dma((halves, R)), dma((halves, R)), dma((halves, G)), dma((halves, G)), dma((halves, R)), dma((halves, R)),
            dma((2,)), dma((halves, mu_dev)), dma((mu_dev,)), dma(()),
            dma(()), dma(()), dma((G, mu_dev)), dma((G, mu_dev)), dma(()), dma(()),
        ],
        compiler_params=pltpu.CompilerParams(
            collective_id=0, has_side_effects=True, vmem_limit_bytes=44 * 1024 * 1024
        ),
        name="fused_exchange",
    )(pivots, columns, previous, inverse, orbitals)


def block_kernel(part_ref, slab_ref, made_ref, out_ref, new_hbm, part_v, spread_ref, new_sem):
    mus, vecs, _ = part_ref.shape
    groups, _, _, j = out_ref.shape
    lot = vecs // groups
    wide = mus * lot
    step = pl.program_id(0)
    store = pltpu.make_async_copy(made_ref, new_hbm, new_sem)

    @pl.when(step == 0)
    def _():
        store.start()
        mu = lax.broadcasted_iota(jnp.int32, (mus, wide), 0)
        col = lax.broadcasted_iota(jnp.int32, (mus, wide), 1)
        repeat = jnp.where(lax.shift_right_logical(col, lot.bit_length() - 1) == mu, 1.0, 0.0).astype(BF16)
        spread_ref[...] = lax.dot_general(
            slab_ref[...], repeat, (((0,), (0,)), ((), ())), preferred_element_type=F32
        ).astype(BF16)
        for k in range(groups):
            part_v[:, k * j : (k + 1) * j] = part_ref[:, k * lot : (k + 1) * lot, :].reshape(wide, j)

    col = lax.broadcasted_iota(jnp.int32, spread_ref.shape, 1) & (lot - 1)
    kept = jnp.where(col == step, spread_ref[...].astype(F32), 0.0).astype(BF16)
    for k in range(groups):
        out_ref[k, 0] = jnp.dot(kept, part_v[:, k * j : (k + 1) * j], preferred_element_type=F32).astype(BF16)

    @pl.when(step == pl.num_programs(0) - 1)
    def _():
        store.wait()


def orbital_block(part, slab, made):
    mus, vecs, j = part.shape
    i = slab.shape[1]
    lot = 8
    assert vecs % lot == 0
    out, new = pl.pallas_call(
        block_kernel,
        grid=(lot,),
        out_shape=(
            jax.ShapeDtypeStruct((vecs // lot, lot, i, j), BF16),
            jax.ShapeDtypeStruct(made.shape, BF16),
        ),
        in_specs=[
            pl.BlockSpec(memory_space=pltpu.VMEM),
            pl.BlockSpec((mus, i), lambda s: (0, 0)),
            pl.BlockSpec(memory_space=pltpu.VMEM),
        ],
        out_specs=(
            pl.BlockSpec((vecs // lot, 1, i, j), lambda s: (0, s, 0, 0)), pl.BlockSpec(memory_space=pl.ANY)
        ),
        scratch_shapes=[
            pltpu.VMEM((mus * lot, vecs // lot * j), BF16),
            pltpu.VMEM((i, mus * lot), BF16),
            pltpu.SemaphoreType.DMA(()),
        ],
        compiler_params=pltpu.CompilerParams(vmem_limit_bytes=40 * 1024 * 1024),
        name="orbital_block",
    )(part, slab, made)
    return out.reshape(vecs, i, j), new


def per_device(R, G, pivot_columns, previous, pivots, pivot_inverse, orbitals, slab_orbitals):
    count = pivot_columns.shape[2]
    stay = functools.partial(pltpu.with_memory_space_constraint, memory_space=pltpu.HBM)
    part, made = fused(
        stay(pivots.reshape(1, count)), pivot_columns, previous, stay(pivot_inverse), orbitals, R, G
    )
    mo_block, new_vectors = orbital_block(part, slab_orbitals, made)
    return new_vectors, mo_block


def solution(mesh):
    R, G = mesh.shape["rows"], mesh.shape["grp"]
    in_specs = (P("rows", "grp", None), P("rows", "grp", None), P(), P(), P("grp", None), P())
    out_specs = (P("rows", "grp", None), P("rows", None, "grp"))
    return jax.shard_map(
        functools.partial(per_device, R, G), mesh=mesh, in_specs=in_specs, out_specs=out_specs,
        check_vma=False,
    )
```

```python
import functools

import jax
import jax.numpy as jnp
from jax import lax
from jax.experimental import pallas as pl
from jax.experimental.pallas import tpu as pltpu
from jax.sharding import PartitionSpec as P

F32 = jnp.float32
BF16 = jnp.bfloat16
MESH = pl.DeviceIdType.MESH


def chained(G):
    return G <= 4


def group_orders(G):
    def due(g, d):
        return 2 * (G - 1 - d) + g if d > g else 2 * d + G - 1 - g

    place = max(G - 2, 0)
    orders = [sorted((d for d in range(G) if d != g), key=lambda d: (due(g, d), d)) for g in range(G)]
    return [order[:place] + [g] + order[place:] for g, order in enumerate(orders)], place


def choose(g, values):
    chosen = jnp.int32(values[0])
    for k in range(1, len(values)):
        chosen = jnp.where(g == k, values[k], chosen)
    return chosen


def fused_kernel(
    R, G, piv_hbm, pc_hbm, prev_hbm, inv_hbm, orb_hbm, out_v, new_v,
    piv_v, inv_v, piv_col, hot_v, picked, buf_x, buf_a, buf_b, buf_c, rows_t, upper_v, prev_v, orb_v, orb_t,
    block_v, send, in_up, in_down, last, own_out, last_in, own_in,
    send_a, recv_a, send_b, recv_b, send_c, recv_c, small_sem, prev_sem, pc_sem, orb_sem,
    hop_sem, up_sem, down_sem, last_send, last_recv, own_send, own_recv,
):
    r = lax.axis_index("rows")
    g = lax.axis_index("grp")
    N = R * G
    me = r * G + g
    mu_dev, nu, p = new_v.shape
    _, _, j_dev, _ = send.shape
    halves, _, c, kh = buf_c.shape

    load_piv = pltpu.make_async_copy(piv_hbm, piv_v, small_sem.at[0])
    load_inv = pltpu.make_async_copy(inv_hbm, inv_v, small_sem.at[1])
    load_orb = pltpu.make_async_copy(orb_hbm, orb_v, orb_sem)

    def load_prev(h, mu):
        at = pl.ds(h * kh, kh)
        return pltpu.make_async_copy(prev_hbm.at[mu, :, at], prev_v.at[mu, :, at], prev_sem.at[h, mu])

    def load_pc(mu):
        return pltpu.make_async_copy(pc_hbm.at[mu], new_v.at[mu], pc_sem.at[mu])

    load_piv.start()
    barrier = pltpu.get_barrier_semaphore()

    @pl.loop(1, N)
    def _(d):
        peer = lax.rem(me + d, N)
        pl.semaphore_signal(
            barrier, inc=1, device_id={"rows": peer // G, "grp": lax.rem(peer, G)}, device_id_type=MESH
        )

    load_piv.wait()
    for h in range(halves):
        for mu in range(mu_dev):
            load_prev(h, mu).start()
    load_inv.start()

    lanes = piv_col.shape[1]
    piv_col[...] = jnp.broadcast_to(piv_v[...], (lanes, p)).T

    def heat(mu):
        base = (r * mu_dev + mu) * (nu * G) + g * nu

        @pl.loop(0, nu // lanes)
        def _(i):
            start = pl.multiple_of(i * lanes, lanes)
            at = lax.broadcasted_iota(jnp.int32, (p, lanes), 1) + (base + start)
            hot_v[mu, :, pl.ds(start, lanes)] = jnp.where(piv_col[...] == at, 1.0, 0.0).astype(BF16)

    def remote(src, dst, send, recv, row, grp):
        return pltpu.make_async_remote_copy(
            src_ref=src, dst_ref=dst, send_sem=send, recv_sem=recv,
            device_id={"rows": row, "grp": grp}, device_id_type=MESH,
        )

    row_peers = [(d, lax.rem(r + d, R)) for d in range(1, R)]
    grp_peers = [(d, lax.rem(g + d, G)) for d in range(1, G)]

    def pick(h):
        picked[...] = jnp.zeros(picked.shape, F32)

        @pl.loop(0, mu_dev)
        def _(mu):
            if h == 0:
                heat(mu)
            load_prev(h, mu).wait()
            picked[...] += jnp.dot(hot_v[mu], prev_v[mu, :, h * kh : (h + 1) * kh], preferred_element_type=F32)

        for k in range(R):
            buf_x[h, k] = picked[k * c : (k + 1) * c, :].astype(BF16)

    def first(h):
        return [
            remote(buf_x.at[h, q], buf_a.at[h, d], send_a.at[h, d], recv_a.at[h, d], q, g) for d, q in row_peers
        ]

    def second(h):
        return [
            remote(buf_b.at[h, 0], buf_b.at[h, d], send_b.at[h, d], recv_b.at[h, d], r, q) for d, q in grp_peers
        ]

    def third(h):
        return [
            remote(buf_c.at[h, r], buf_c.at[h, r], send_c.at[h, d], recv_c.at[h, d], q, g) for d, q in row_peers
        ]

    def add_rows(h):
        total = buf_x[h, r].astype(F32)
        for (d, _), copy in zip(row_peers, first(h)):
            copy.wait_recv()
            total = total + buf_a[h, d].astype(F32)
        buf_b[h, 0] = total.astype(BF16)
        for copy in second(h):
            copy.start()

    def add_groups(h):
        total = buf_b[h, 0].astype(F32)
        for (d, _), copy in zip(grp_peers, second(h)):
            copy.wait_recv()
            total = total + buf_b[h, d].astype(F32)
        buf_c[h, r] = total.astype(BF16)
        for copy in third(h):
            copy.start()

    def take_rows(h):
        for copy in third(h):
            copy.wait_recv()
        for k in range(R):
            picked[k * c : (k + 1) * c, :] = buf_c[h, k].astype(F32)
        rows_t[h * kh : (h + 1) * kh, :] = picked[...].T.astype(BF16)

    square = (256, 256)
    eye = jnp.where(
        lax.broadcasted_iota(jnp.int32, square, 0) == lax.broadcasted_iota(jnp.int32, square, 1), 1.0, 0.0
    ).astype(BF16)
    wide = orb_v.shape[1] // 256

    def turn_orbitals(first, last):
        @pl.loop(first, last)
        def _(i):
            at = pl.ds(pl.multiple_of(i * 256, 256), 256)
            for q in range(wide):
                orb_t[q * 256 : (q + 1) * 256, at] = lax.dot_general(
                    eye, orb_v[at, q * 256 : (q + 1) * 256], (((1,), (1,)), ((), ())), preferred_element_type=F32
                ).astype(BF16)

    tiles = nu // 256
    cuts = [tiles * k // (2 * halves) for k in range(2 * halves + 1)]
    for h in range(halves):
        pick(h)
        if h == 0:
            load_orb.start()
            for mu in range(mu_dev):
                load_pc(mu).start()
            pl.semaphore_wait(barrier, N - 1)
        for copy in first(h):
            copy.start()
    load_inv.wait()
    low = lax.broadcasted_iota(jnp.int32, (p, p), 0)
    high = lax.broadcasted_iota(jnp.int32, (p, p), 1)
    upper_v[...] = jnp.where(low <= high, inv_v[...].astype(F32), 0.0).astype(BF16)
    load_orb.wait()
    for h in range(halves):
        add_rows(h)
        turn_orbitals(cuts[h], cuts[h + 1])
    for h in range(halves):
        add_groups(h)
        turn_orbitals(cuts[halves + h], cuts[halves + h + 1])
    for h in range(halves):
        take_rows(h)

    chunk = 512 if nu % 512 == 0 else 256
    orders, place = group_orders(G)

    def make_vectors(mu):
        load_pc(mu).wait()
        for i in range(nu // chunk):
            at = pl.ds(i * chunk, chunk)
            correction = jnp.dot(prev_v[mu, at, :], rows_t[...], preferred_element_type=F32)
            residual = (new_v[mu, at, :].astype(F32) - correction).astype(BF16)
            new_v[mu, at, :] = jnp.dot(residual, upper_v[...], preferred_element_type=F32).astype(BF16)

    def add(buf, slot, sem, mu):
        here = buf.at[slot, mu]
        pltpu.make_async_copy(here, here, sem.at[slot, mu]).wait()
        block_v[...] += buf[slot, mu].astype(F32)

    def hand_out(mu, src, dst, send, recv, grp):
        for k in range(R):
            peer = lax.rem(r + k, R)
            remote(src.at[peer], dst.at[r * mu_dev + mu], send, recv, peer, grp).start()

    for s in range(G):
        to = choose(g, [order[s] for order in orders])

        @pl.loop(0, mu_dev)
        def _(mu):
            if s == 0:
                make_vectors(mu)
            at = pl.ds(pl.multiple_of(to * j_dev, j_dev), j_dev)
            block_v[...] = jnp.dot(orb_t[at, :], new_v[mu], preferred_element_type=F32)
            if s == place:
                whole = block_v[...].T
                for k in range(R):
                    own_out[mu, k] = whole[k * c : (k + 1) * c, :]
                own_in[r * mu_dev + mu] = own_out[mu, r]
                for k in range(1, R):
                    peer = lax.rem(r + k, R)
                    remote(
                        own_out.at[mu, peer], own_in.at[r * mu_dev + mu], own_send, own_recv, peer, g
                    ).start()
                return
            if not chained(G):
                turned = block_v[...].T.astype(BF16)
                slot = s - (s > place)
                for k in range(R):
                    last[slot, mu, k] = turned[k * c : (k + 1) * c, :]
                hand_out(mu, last.at[slot, mu], last_in.at[g], last_send, last_recv.at[g], to)
                return
            pl.when((to > g) & (g > 0))(lambda: add(in_up, to, up_sem, mu))
            pl.when((to < g) & (g < G - 1))(lambda: add(in_down, to, down_sem, mu))
            next_up = to == g + 1
            next_down = to == g - 1

            @pl.when(next_up | next_down)
            def _():
                slot = jnp.where(next_up, 0, 1)
                turned = block_v[...].T.astype(BF16)
                for k in range(R):
                    last[slot, mu, k] = turned[k * c : (k + 1) * c, :]
                hand_out(mu, last.at[slot, mu], last_in.at[slot], last_send, last_recv.at[slot], to)

            @pl.when(jnp.logical_not(next_up | next_down))
            def _():
                send[to, mu] = block_v[...].astype(BF16)

                @pl.when(to > g)
                def _():
                    remote(send.at[to, mu], in_up.at[to, mu], hop_sem, up_sem.at[to, mu], r, g + 1).start()

                @pl.when(to < g)
                def _():
                    remote(send.at[to, mu], in_down.at[to, mu], hop_sem, down_sem.at[to, mu], r, g - 1).start()

    def take(copy, when):
        pl.when(when)(copy.wait)

    def gather(slot, when):
        everything = last_in.at[slot]
        take(pltpu.make_async_copy(everything, everything, last_recv.at[slot]), when)

        @pl.when(when)
        def _():
            own_in[...] += last_in[slot].astype(F32)

    others = own_in.at[pl.ds(0, (R - 1) * mu_dev)]
    pltpu.make_async_copy(others, others, own_recv).wait()
    if chained(G):
        early = g >= G // 2
        gather(0, (g > 0) & early)
        gather(1, g < G - 1)
        gather(0, (g > 0) & jnp.logical_not(early))
    else:
        for slot in range(G):
            gather(slot, g != slot)
    out_v[...] = own_in[...].astype(BF16)

    for h in range(halves):
        for copy in first(h) + second(h) + third(h):
            copy.wait_send()
    pltpu.make_async_copy(others, others, own_send).wait()
    if chained(G):
        ends = (g > 0).astype(jnp.int32) + (g < G - 1).astype(jnp.int32)
        for count in range(1, 3):
            near = last.at[pl.ds(0, count)]
            take(pltpu.make_async_copy(near, near, last_send), ends == count)
            if G - 1 > count:
                far = send.at[pl.ds(0, G - 1 - count)]
                take(pltpu.make_async_copy(far, far, hop_sem), ends == count)
    else:
        pltpu.make_async_copy(last, last, last_send).wait()


def fused(pivots, columns, previous, inverse, orbitals, R, G):
    mu_dev, nu, p = columns.shape
    k = previous.shape[2]
    c = p // R
    nj = orbitals.shape[1]
    halves = 2
    kh = k // halves
    hbm = pl.BlockSpec(memory_space=pltpu.HBM)
    slots = 2 if chained(G) else G
    relays = G if chained(G) else 1
    blocks = (R * mu_dev, c, nj // G)
    vmem = pl.BlockSpec(memory_space=pltpu.VMEM)
    dma = pltpu.SemaphoreType.DMA
    return pl.pallas_call(
        functools.partial(fused_kernel, R, G),
        out_shape=(
            jax.ShapeDtypeStruct(blocks, BF16),
            jax.ShapeDtypeStruct(columns.shape, BF16),
        ),
        in_specs=[hbm, hbm, hbm, hbm, hbm],
        out_specs=(vmem, vmem),
        scratch_shapes=[
            pltpu.VMEM((1, p), jnp.int32),
            pltpu.VMEM((p, p), BF16),
            pltpu.VMEM((p, 128), jnp.int32),
            pltpu.VMEM((mu_dev, p, nu), BF16),
            pltpu.VMEM((p, kh), F32),
            pltpu.VMEM((halves, R, c, kh), BF16),
            pltpu.VMEM((halves, R, c, kh), BF16),
            pltpu.VMEM((halves, G, c, kh), BF16),
            pltpu.VMEM((halves, R, c, kh), BF16),
            pltpu.VMEM((k, p), BF16),
            pltpu.VMEM((p, p), BF16),
            pltpu.VMEM((mu_dev, nu, k), BF16),
            pltpu.VMEM((nu, nj), BF16),
            pltpu.VMEM((nj, nu), BF16),
            pltpu.VMEM((nj // G, p), F32),
            pltpu.VMEM((relays, mu_dev, nj // G, p), BF16),
            pltpu.VMEM((relays, mu_dev, nj // G, p), BF16),
            pltpu.VMEM((relays, mu_dev, nj // G, p), BF16),
            pltpu.VMEM((2 if chained(G) else G - 1, mu_dev, R, c, nj // G), BF16),
            pltpu.VMEM((mu_dev, R, c, nj // G), F32),
            pltpu.VMEM((slots,) + blocks, BF16),
            pltpu.VMEM(blocks, F32),
            dma((halves, R)), dma((halves, R)), dma((halves, G)), dma((halves, G)), dma((halves, R)), dma((halves, R)),
            dma((2,)), dma((halves, mu_dev)), dma((mu_dev,)), dma(()),
            dma(()), dma((G, mu_dev)), dma((G, mu_dev)), dma(()), dma((slots,)), dma(()), dma(()),
        ],
        compiler_params=pltpu.CompilerParams(
            collective_id=0, has_side_effects=True, vmem_limit_bytes=44 * 1024 * 1024
        ),
        name="fused_exchange",
    )(pivots, columns, previous, inverse, orbitals)


def block_kernel(part_ref, slab_ref, made_ref, out_hbm, new_hbm, out_v, part_v, spread_ref, new_sem, out_sem):
    mus, vecs, j = part_ref.shape
    groups, lot, _, _ = out_v.shape
    wide = mus * lot
    store = pltpu.make_async_copy(made_ref, new_hbm, new_sem)
    store.start()
    mu = lax.broadcasted_iota(jnp.int32, (mus, wide), 0)
    col = lax.broadcasted_iota(jnp.int32, (mus, wide), 1)
    repeat = jnp.where(lax.shift_right_logical(col, lot.bit_length() - 1) == mu, 1.0, 0.0).astype(BF16)
    spread_ref[...] = lax.dot_general(
        slab_ref[...], repeat, (((0,), (0,)), ((), ())), preferred_element_type=F32
    ).astype(BF16)
    for k in range(groups):
        part_v[k] = part_ref[:, k * lot : (k + 1) * lot, :].reshape(wide, j)

    def piece(q, k):
        return pltpu.make_async_copy(out_v.at[k, q], out_hbm.at[k, q], out_sem.at[k, q])

    @pl.loop(0, lot)
    def _(q):
        at = lax.broadcasted_iota(jnp.int32, spread_ref.shape, 1) & (lot - 1)
        kept = jnp.where(at == q, spread_ref[...].astype(F32), 0.0).astype(BF16)
        for k in range(groups):
            out_v[k, q] = jnp.dot(kept, part_v[k], preferred_element_type=F32).astype(BF16)
            piece(q, k).start()

    @pl.loop(0, lot)
    def _(q):
        for k in range(groups):
            piece(q, k).wait()
    store.wait()


def orbital_block(part, slab, made):
    mus, vecs, j = part.shape
    i = slab.shape[1]
    lot = 8
    assert vecs % lot == 0
    groups = vecs // lot
    vmem = pl.BlockSpec(memory_space=pltpu.VMEM)
    anywhere = pl.BlockSpec(memory_space=pl.ANY)
    out, new = pl.pallas_call(
        block_kernel,
        out_shape=(
            jax.ShapeDtypeStruct((groups, lot, i, j), BF16),
            jax.ShapeDtypeStruct(made.shape, BF16),
        ),
        in_specs=[vmem, vmem, vmem],
        out_specs=(anywhere, anywhere),
        scratch_shapes=[
            pltpu.VMEM((groups, lot, i, j), BF16),
            pltpu.VMEM((groups, mus * lot, j), BF16),
            pltpu.VMEM((i, mus * lot), BF16),
            pltpu.SemaphoreType.DMA(()),
            pltpu.SemaphoreType.DMA((groups, lot)),
        ],
        compiler_params=pltpu.CompilerParams(vmem_limit_bytes=40 * 1024 * 1024),
        name="orbital_block",
    )(part, slab, made)
    return out.reshape(vecs, i, j), new


def per_device(R, G, pivot_columns, previous, pivots, pivot_inverse, orbitals, slab_orbitals):
    count = pivot_columns.shape[2]
    stay = functools.partial(pltpu.with_memory_space_constraint, memory_space=pltpu.HBM)
    part, made = fused(
        stay(pivots.reshape(1, count)), pivot_columns, previous, stay(pivot_inverse), orbitals, R, G
    )
    mo_block, new_vectors = orbital_block(part, slab_orbitals, made)
    return new_vectors, mo_block


def solution(mesh):
    R, G = mesh.shape["rows"], mesh.shape["grp"]
    in_specs = (P("rows", "grp", None), P("rows", "grp", None), P(), P(), P("grp", None), P())
    out_specs = (P("rows", "grp", None), P("rows", None, "grp"))
    return jax.shard_map(
        functools.partial(per_device, R, G), mesh=mesh, in_specs=in_specs, out_specs=out_specs,
        check_vma=False,
    )
```

```python
import functools

import jax
import jax.numpy as jnp
from jax import lax
from jax.experimental import pallas as pl
from jax.experimental.pallas import tpu as pltpu
from jax.sharding import PartitionSpec as P

F32 = jnp.float32
BF16 = jnp.bfloat16
MESH = pl.DeviceIdType.MESH


def chained(G):
    return G <= 4


def group_orders(G):
    def due(g, d):
        if d == g:
            return 4 * G if chained(G) and g in (0, G - 1) else -1
        return 2 * (G - 1 - d) + g if d > g else 2 * d + G - 1 - g

    return [sorted(range(G), key=lambda d: (due(g, d), d)) for g in range(G)]


def choose(g, values):
    chosen = jnp.int32(values[0])
    for k in range(1, len(values)):
        chosen = jnp.where(g == k, values[k], chosen)
    return chosen


def fused_kernel(
    R, G, piv_hbm, pc_hbm, prev_hbm, inv_hbm, orb_hbm, out_v, new_v,
    piv_v, inv_v, piv_col, hot_v, picked, buf_x, buf_a, buf_b, buf_c, rows_t, upper_v, prev_v, orb_v, orb_t,
    block_v, send, in_up, in_down, last, own_out, last_in, own_in,
    send_a, recv_a, send_b, recv_b, send_c, recv_c, small_sem, prev_sem, pc_sem, orb_sem,
    hop_sem, up_sem, down_sem, last_send, last_recv, own_send, own_recv,
):
    r = lax.axis_index("rows")
    g = lax.axis_index("grp")
    N = R * G
    me = r * G + g
    mu_dev, nu, p = new_v.shape
    _, _, j_dev, _ = send.shape
    halves, _, c, kh = buf_c.shape

    load_piv = pltpu.make_async_copy(piv_hbm, piv_v, small_sem.at[0])
    load_inv = pltpu.make_async_copy(inv_hbm, inv_v, small_sem.at[1])
    load_orb = pltpu.make_async_copy(orb_hbm, orb_v, orb_sem)

    def load_prev(h, mu):
        at = pl.ds(h * kh, kh)
        return pltpu.make_async_copy(prev_hbm.at[mu, :, at], prev_v.at[mu, :, at], prev_sem.at[h, mu])

    def load_pc(mu):
        return pltpu.make_async_copy(pc_hbm.at[mu], new_v.at[mu], pc_sem.at[mu])

    load_piv.start()
    barrier = pltpu.get_barrier_semaphore()

    @pl.loop(1, N)
    def _(d):
        peer = lax.rem(me + d, N)
        pl.semaphore_signal(
            barrier, inc=1, device_id={"rows": peer // G, "grp": lax.rem(peer, G)}, device_id_type=MESH
        )

    load_piv.wait()
    for h in range(halves):
        for mu in range(mu_dev):
            load_prev(h, mu).start()
    load_inv.start()

    lanes = piv_col.shape[1]
    piv_col[...] = jnp.broadcast_to(piv_v[...], (lanes, p)).T

    def heat(mu):
        base = (r * mu_dev + mu) * (nu * G) + g * nu

        @pl.loop(0, nu // lanes)
        def _(i):
            start = pl.multiple_of(i * lanes, lanes)
            at = lax.broadcasted_iota(jnp.int32, (p, lanes), 1) + (base + start)
            hot_v[mu, :, pl.ds(start, lanes)] = jnp.where(piv_col[...] == at, 1.0, 0.0).astype(BF16)

    for mu in range(mu_dev):
        heat(mu)

    def remote(src, dst, send, recv, row, grp):
        return pltpu.make_async_remote_copy(
            src_ref=src, dst_ref=dst, send_sem=send, recv_sem=recv,
            device_id={"rows": row, "grp": grp}, device_id_type=MESH,
        )

    row_peers = [(d, lax.rem(r + d, R)) for d in range(1, R)]
    grp_peers = [(d, lax.rem(g + d, G)) for d in range(1, G)]

    def pick(h):
        picked[...] = jnp.zeros(picked.shape, F32)

        @pl.loop(0, mu_dev)
        def _(mu):
            load_prev(h, mu).wait()
            picked[...] += jnp.dot(hot_v[mu], prev_v[mu, :, h * kh : (h + 1) * kh], preferred_element_type=F32)

        for k in range(R):
            buf_x[h, k] = picked[k * c : (k + 1) * c, :].astype(BF16)

    def first(h):
        return [
            remote(buf_x.at[h, q], buf_a.at[h, d], send_a.at[h, d], recv_a.at[h, d], q, g) for d, q in row_peers
        ]

    def second(h):
        return [
            remote(buf_b.at[h, 0], buf_b.at[h, d], send_b.at[h, d], recv_b.at[h, d], r, q) for d, q in grp_peers
        ]

    def third(h):
        return [
            remote(buf_c.at[h, r], buf_c.at[h, r], send_c.at[h, d], recv_c.at[h, d], q, g) for d, q in row_peers
        ]

    def add_rows(h):
        total = buf_x[h, r].astype(F32)
        for (d, _), copy in zip(row_peers, first(h)):
            copy.wait_recv()
            total = total + buf_a[h, d].astype(F32)
        buf_b[h, 0] = total.astype(BF16)
        for copy in second(h):
            copy.start()

    def add_groups(h):
        total = buf_b[h, 0].astype(F32)
        for (d, _), copy in zip(grp_peers, second(h)):
            copy.wait_recv()
            total = total + buf_b[h, d].astype(F32)
        buf_c[h, r] = total.astype(BF16)
        for copy in third(h):
            copy.start()

    def take_rows(h):
        for copy in third(h):
            copy.wait_recv()
        for k in range(R):
            picked[k * c : (k + 1) * c, :] = buf_c[h, k].astype(F32)
        rows_t[h * kh : (h + 1) * kh, :] = picked[...].T.astype(BF16)

    square = (256, 256)
    eye = jnp.where(
        lax.broadcasted_iota(jnp.int32, square, 0) == lax.broadcasted_iota(jnp.int32, square, 1), 1.0, 0.0
    ).astype(BF16)
    wide = orb_v.shape[1] // 256

    def turn_orbitals(first, last):
        @pl.loop(first, last)
        def _(i):
            at = pl.ds(pl.multiple_of(i * 256, 256), 256)
            for q in range(wide):
                orb_t[q * 256 : (q + 1) * 256, at] = lax.dot_general(
                    eye, orb_v[at, q * 256 : (q + 1) * 256], (((1,), (1,)), ((), ())), preferred_element_type=F32
                ).astype(BF16)

    tiles = nu // 256
    cuts = [tiles * k // (2 * halves) for k in range(2 * halves + 1)]
    for h in range(halves):
        pick(h)
        if h == 0:
            load_orb.start()
            for mu in range(mu_dev):
                load_pc(mu).start()
            pl.semaphore_wait(barrier, N - 1)
        for copy in first(h):
            copy.start()
    load_inv.wait()
    low = lax.broadcasted_iota(jnp.int32, (p, p), 0)
    high = lax.broadcasted_iota(jnp.int32, (p, p), 1)
    upper_v[...] = jnp.where(low <= high, inv_v[...].astype(F32), 0.0).astype(BF16)
    for h in range(halves):
        add_rows(h)
        if h == 0:
            load_orb.wait()
        turn_orbitals(cuts[h], cuts[h + 1])
    for h in range(halves):
        add_groups(h)
        turn_orbitals(cuts[halves + h], cuts[halves + h + 1])
    for h in range(halves):
        take_rows(h)

    chunk = nu // 2
    orders = group_orders(G)

    def make_vectors(mu):
        load_pc(mu).wait()
        parts = [pl.ds(i * chunk, chunk) for i in range(nu // chunk)]
        left = []
        for at in parts:
            correction = jnp.dot(prev_v[mu, at, :], rows_t[...], preferred_element_type=F32)
            left.append((new_v[mu, at, :].astype(F32) - correction).astype(BF16))
        for at, residual in zip(parts, left):
            new_v[mu, at, :] = jnp.dot(residual, upper_v[...], preferred_element_type=F32).astype(BF16)

    def add(buf, slot, sem, mu):
        here = buf.at[slot, mu]
        pltpu.make_async_copy(here, here, sem.at[slot, mu]).wait()
        block_v[...] += buf[slot, mu].astype(F32)

    def hand_out(mu, src, dst, send, recv, grp):
        for k in range(R):
            peer = lax.rem(r + k, R)
            remote(src.at[peer], dst.at[r * mu_dev + mu], send, recv, peer, grp).start()

    at_low = g == 0
    at_high = g == G - 1
    at_end = (at_low | at_high) & chained(G)

    def emit(to, mu):
        own = to == g
        if chained(G):
            pl.when(jnp.logical_not(at_low) & ((to > g) | (own & at_high)))(lambda: add(in_up, to, up_sem, mu))
            pl.when(jnp.logical_not(at_high) & ((to < g) | (own & at_low)))(lambda: add(in_down, to, down_sem, mu))
            near = ((to == g + 1) & (to < G - 1)) | ((to == g - 1) & (to > 0))
        else:
            near = jnp.logical_not(own)

        @pl.when(own & jnp.logical_not(at_end))
        def _():
            whole = block_v[...].T
            for k in range(R):
                own_out[mu, k] = whole[k * c : (k + 1) * c, :]
            own_in[r * mu_dev + mu] = own_out[mu, r]
            for k in range(1, R):
                peer = lax.rem(r + k, R)
                remote(own_out.at[mu, peer], own_in.at[r * mu_dev + mu], own_send, own_recv, peer, g).start()

        def turn_last(slot):
            turned = block_v[...].T.astype(BF16)
            for k in range(R):
                last[slot, mu, k] = turned[k * c : (k + 1) * c, :]

        @pl.when(near)
        def _():
            if chained(G):
                slot = jnp.where(to > g, 0, 1)
                into = slot
            else:
                slot = to - (to > g).astype(jnp.int32)
                into = g
            turn_last(slot)
            for k in range(R):
                peer = lax.rem(r + k, R)
                remote(
                    last.at[slot, mu, peer], last_in.at[into, r * mu_dev + mu], last_send, last_recv.at[into], peer, to
                ).start()

        if not chained(G):
            return

        @pl.when(own & at_end)
        def _():
            slot = jnp.where(at_low, 1, 0)
            turn_last(slot)
            last_in[0, r * mu_dev + mu] = last[slot, mu, r]
            for k in range(1, R):
                peer = lax.rem(r + k, R)
                remote(
                    last.at[slot, mu, peer], last_in.at[0, r * mu_dev + mu], own_send, last_recv.at[0], peer, g
                ).start()

        @pl.when(jnp.logical_not(own | near))
        def _():
            send[to, mu] = block_v[...].astype(BF16)

            @pl.when(to > g)
            def _():
                remote(send.at[to, mu], in_up.at[to, mu], hop_sem, up_sem.at[to, mu], r, g + 1).start()

            @pl.when(to < g)
            def _():
                remote(send.at[to, mu], in_down.at[to, mu], hop_sem, down_sem.at[to, mu], r, g - 1).start()

    def block(to, mu):
        at = pl.ds(pl.multiple_of(to * j_dev, j_dev), j_dev)
        block_v[...] = jnp.dot(orb_t[at, :], new_v[mu], preferred_element_type=F32)

    initial = choose(g, [order[0] for order in orders])

    @pl.loop(0, mu_dev)
    def _(mu):
        make_vectors(mu)
        block(initial, mu)
        emit(initial, mu)

    for s in range(1, G):
        to = choose(g, [order[s] for order in orders])

        @pl.loop(0, mu_dev)
        def _(mu):
            block(to, mu)
            emit(to, mu)

    def take(buf, sem, when):
        pl.when(when)(pltpu.make_async_copy(buf, buf, sem).wait)

    def gather(slot, when):
        take(last_in.at[slot], last_recv.at[slot], when)

        @pl.when(when)
        def _():
            own_in[...] += last_in[slot].astype(F32)

    inner = jnp.logical_not(at_end)
    others = own_in.at[pl.ds(0, (R - 1) * mu_dev)]
    take(others, own_recv, inner)
    if chained(G):
        gather(0, inner & (2 * g >= G))
        gather(1, inner)
        gather(0, inner & (2 * g < G))
        rounded = last_in.at[0, pl.ds(0, (R - 1) * mu_dev)]
        take(rounded, last_recv.at[0], at_end)

        @pl.when(at_end)
        def _():
            out_v[...] = last_in[0]
    else:
        for slot in range(G):
            gather(slot, g != slot)

    @pl.when(inner)
    def _():
        out_v[...] = own_in[...].astype(BF16)

    for h in range(halves):
        for copy in first(h) + second(h) + third(h):
            copy.wait_send()
    take(others, own_send, inner)
    if chained(G):
        take(rounded, own_send, at_end)
        nears = (g + 1 < G - 1).astype(jnp.int32) + (g - 1 > 0).astype(jnp.int32)
        for count in range(3):
            if count:
                take(last.at[pl.ds(0, count)], last_send, nears == count)
            if G - 1 > count:
                take(send.at[pl.ds(0, G - 1 - count)], hop_sem, nears == count)
    else:
        take(last, last_send, inner)


def fused(pivots, columns, previous, inverse, orbitals, R, G):
    mu_dev, nu, p = columns.shape
    k = previous.shape[2]
    c = p // R
    nj = orbitals.shape[1]
    halves = 2
    kh = k // halves
    hbm = pl.BlockSpec(memory_space=pltpu.HBM)
    slots = 2 if chained(G) else G
    relays = G if chained(G) else 1
    blocks = (R * mu_dev, c, nj // G)
    vmem = pl.BlockSpec(memory_space=pltpu.VMEM)
    dma = pltpu.SemaphoreType.DMA
    return pl.pallas_call(
        functools.partial(fused_kernel, R, G),
        out_shape=(
            jax.ShapeDtypeStruct(blocks, BF16),
            jax.ShapeDtypeStruct(columns.shape, BF16),
        ),
        in_specs=[hbm, hbm, hbm, hbm, hbm],
        out_specs=(vmem, vmem),
        scratch_shapes=[
            pltpu.VMEM((1, p), jnp.int32),
            pltpu.VMEM((p, p), BF16),
            pltpu.VMEM((p, 128), jnp.int32),
            pltpu.VMEM((mu_dev, p, nu), BF16),
            pltpu.VMEM((p, kh), F32),
            pltpu.VMEM((halves, R, c, kh), BF16),
            pltpu.VMEM((halves, R, c, kh), BF16),
            pltpu.VMEM((halves, G, c, kh), BF16),
            pltpu.VMEM((halves, R, c, kh), BF16),
            pltpu.VMEM((k, p), BF16),
            pltpu.VMEM((p, p), BF16),
            pltpu.VMEM((mu_dev, nu, k), BF16),
            pltpu.VMEM((nu, nj), BF16),
            pltpu.VMEM((nj, nu), BF16),
            pltpu.VMEM((nj // G, p), F32),
            pltpu.VMEM((relays, mu_dev, nj // G, p), BF16),
            pltpu.VMEM((relays, mu_dev, nj // G, p), BF16),
            pltpu.VMEM((relays, mu_dev, nj // G, p), BF16),
            pltpu.VMEM((2 if chained(G) else G - 1, mu_dev, R, c, nj // G), BF16),
            pltpu.VMEM((mu_dev, R, c, nj // G), F32),
            pltpu.VMEM((slots,) + blocks, BF16),
            pltpu.VMEM(blocks, F32),
            dma((halves, R)), dma((halves, R)), dma((halves, G)), dma((halves, G)), dma((halves, R)), dma((halves, R)),
            dma((2,)), dma((halves, mu_dev)), dma((mu_dev,)), dma(()),
            dma(()), dma((G, mu_dev)), dma((G, mu_dev)), dma(()), dma((slots,)), dma(()), dma(()),
        ],
        compiler_params=pltpu.CompilerParams(
            collective_id=0, has_side_effects=True, vmem_limit_bytes=44 * 1024 * 1024
        ),
        name="fused_exchange",
    )(pivots, columns, previous, inverse, orbitals)


def block_kernel(part_ref, slab_ref, made_ref, out_hbm, new_hbm, out_v, part_v, spread_ref, new_sem, out_sem):
    mus, vecs, j = part_ref.shape
    groups, lot, _, _ = out_v.shape
    wide = mus * lot
    store = pltpu.make_async_copy(made_ref, new_hbm, new_sem)
    store.start()
    mu = lax.broadcasted_iota(jnp.int32, (mus, wide), 0)
    col = lax.broadcasted_iota(jnp.int32, (mus, wide), 1)
    repeat = jnp.where(lax.shift_right_logical(col, lot.bit_length() - 1) == mu, 1.0, 0.0).astype(BF16)
    spread_ref[...] = lax.dot_general(
        slab_ref[...], repeat, (((0,), (0,)), ((), ())), preferred_element_type=F32
    ).astype(BF16)
    for k in range(groups):
        part_v[k] = part_ref[:, k * lot : (k + 1) * lot, :].reshape(wide, j)

    def piece(q, k):
        return pltpu.make_async_copy(out_v.at[k, q], out_hbm.at[k, q], out_sem.at[k, q])

    @pl.loop(0, lot)
    def _(q):
        at = lax.broadcasted_iota(jnp.int32, spread_ref.shape, 1) & (lot - 1)
        kept = jnp.where(at == q, spread_ref[...].astype(F32), 0.0).astype(BF16)
        for k in range(groups):
            out_v[k, q] = jnp.dot(kept, part_v[k], preferred_element_type=F32).astype(BF16)
            piece(q, k).start()

    @pl.loop(0, lot)
    def _(q):
        for k in range(groups):
            piece(q, k).wait()
    store.wait()


def orbital_block(part, slab, made):
    mus, vecs, j = part.shape
    i = slab.shape[1]
    lot = 8
    assert vecs % lot == 0
    groups = vecs // lot
    vmem = pl.BlockSpec(memory_space=pltpu.VMEM)
    anywhere = pl.BlockSpec(memory_space=pl.ANY)
    out, new = pl.pallas_call(
        block_kernel,
        out_shape=(
            jax.ShapeDtypeStruct((groups, lot, i, j), BF16),
            jax.ShapeDtypeStruct(made.shape, BF16),
        ),
        in_specs=[vmem, vmem, vmem],
        out_specs=(anywhere, anywhere),
        scratch_shapes=[
            pltpu.VMEM((groups, lot, i, j), BF16),
            pltpu.VMEM((groups, mus * lot, j), BF16),
            pltpu.VMEM((i, mus * lot), BF16),
            pltpu.SemaphoreType.DMA(()),
            pltpu.SemaphoreType.DMA((groups, lot)),
        ],
        compiler_params=pltpu.CompilerParams(vmem_limit_bytes=40 * 1024 * 1024),
        name="orbital_block",
    )(part, slab, made)
    return out.reshape(vecs, i, j), new


def per_device(R, G, pivot_columns, previous, pivots, pivot_inverse, orbitals, slab_orbitals):
    count = pivot_columns.shape[2]
    stay = functools.partial(pltpu.with_memory_space_constraint, memory_space=pltpu.HBM)
    part, made = fused(
        stay(pivots.reshape(1, count)), pivot_columns, previous, stay(pivot_inverse), orbitals, R, G
    )
    mo_block, new_vectors = orbital_block(part, slab_orbitals, made)
    return new_vectors, mo_block


def solution(mesh):
    R, G = mesh.shape["rows"], mesh.shape["grp"]
    in_specs = (P("rows", "grp", None), P("rows", "grp", None), P(), P(), P("grp", None), P())
    out_specs = (P("rows", "grp", None), P("rows", None, "grp"))
    return jax.shard_map(
        functools.partial(per_device, R, G), mesh=mesh, in_specs=in_specs, out_specs=out_specs,
        check_vma=False,
    )
```

```python
import functools

import jax
import jax.numpy as jnp
from jax import lax
from jax.experimental import pallas as pl
from jax.experimental.pallas import tpu as pltpu
from jax.sharding import PartitionSpec as P

F32 = jnp.float32
BF16 = jnp.bfloat16
MESH = pl.DeviceIdType.MESH


def chained(G):
    return G <= 4


def group_orders(G):
    def due(g, d):
        if d == g:
            return 4 * G if chained(G) and g in (0, G - 1) else -1
        return 2 * (G - 1 - d) + g if d > g else 2 * d + G - 1 - g

    return [sorted(range(G), key=lambda d: (due(g, d), d)) for g in range(G)]


def choose(g, values):
    chosen = jnp.int32(values[0])
    for k in range(1, len(values)):
        chosen = jnp.where(g == k, values[k], chosen)
    return chosen


def fused_kernel(
    R, G, piv_hbm, pc_hbm, prev_hbm, inv_hbm, orb_hbm, out_v, new_v,
    piv_v, inv_v, piv_col, hot_v, picked, buf_x, buf_a, buf_b, buf_c, rows_t, upper_v, prev_v, orb_v, orb_t,
    block_v, begun, send, in_up, in_down, last, own_out, last_in, own_in,
    send_a, recv_a, send_b, recv_b, send_c, recv_c, small_sem, prev_sem, pc_sem, orb_sem,
    hop_sem, up_sem, down_sem, last_send, last_recv, own_send, own_recv,
):
    r = lax.axis_index("rows")
    g = lax.axis_index("grp")
    mu_dev, nu, p = new_v.shape
    _, _, j_dev, _ = send.shape
    halves, _, c, kh = buf_c.shape

    load_piv = pltpu.make_async_copy(piv_hbm, piv_v, small_sem.at[0])
    load_inv = pltpu.make_async_copy(inv_hbm, inv_v, small_sem.at[1])
    load_orb = pltpu.make_async_copy(orb_hbm, orb_v, orb_sem)

    def load_prev(h, mu):
        at = pl.ds(h * kh, kh)
        return pltpu.make_async_copy(prev_hbm.at[mu, :, at], prev_v.at[mu, :, at], prev_sem.at[h, mu])

    def load_pc(mu):
        return pltpu.make_async_copy(pc_hbm.at[mu], new_v.at[mu], pc_sem.at[mu])

    load_piv.start()
    barrier = pltpu.get_barrier_semaphore()

    def greet(row, grp):
        pl.semaphore_signal(barrier, inc=1, device_id={"rows": row, "grp": grp}, device_id_type=MESH)

    def greet_rows(step):
        @pl.loop(1, R)
        def _(d):
            greet(lax.rem(r + d, R), lax.rem(g + step + G, G))

    greet_rows(0)
    for d in range(1, G):
        greet(r, lax.rem(g + d, G))
    if chained(G):
        if G > 1:
            pl.when(g > 0)(lambda: greet_rows(-1))
            pl.when(g < G - 1)(lambda: greet_rows(1))
        sides = (g > 0).astype(jnp.int32) + (g < G - 1).astype(jnp.int32)
    else:
        for d in range(1, G):
            greet_rows(d)
        sides = G - 1
    greetings = (sides + 1) * (R - 1) + G - 1
    for h in range(halves):
        for mu in range(mu_dev):
            load_prev(h, mu).start()
    load_inv.start()
    load_piv.wait()

    lanes = piv_col.shape[1]
    piv_col[...] = jnp.broadcast_to(piv_v[...], (lanes, p)).T

    def heat(mu):
        base = (r * mu_dev + mu) * (nu * G) + g * nu
        for i in range(nu // lanes):
            at = lax.broadcasted_iota(jnp.int32, (p, lanes), 1) + (base + i * lanes)
            hot_v[mu, :, i * lanes : (i + 1) * lanes] = jnp.where(piv_col[...] == at, 1.0, 0.0).astype(BF16)

    def remote(src, dst, send, recv, row, grp):
        return pltpu.make_async_remote_copy(
            src_ref=src, dst_ref=dst, send_sem=send, recv_sem=recv,
            device_id={"rows": row, "grp": grp}, device_id_type=MESH,
        )

    row_peers = [(d, lax.rem(r + d, R)) for d in range(1, R)]
    grp_peers = [(d, lax.rem(g + d, G)) for d in range(1, G)]

    for mu in range(mu_dev):
        heat(mu)

    def pick(h):
        picked[...] = jnp.zeros(picked.shape, F32)

        @pl.loop(0, mu_dev)
        def _(mu):
            load_prev(h, mu).wait()
            picked[...] += jnp.dot(hot_v[mu], prev_v[mu, :, h * kh : (h + 1) * kh], preferred_element_type=F32)

        for k in range(R):
            buf_x[h, k] = picked[k * c : (k + 1) * c, :].astype(BF16)

    def first(h):
        return [
            remote(buf_x.at[h, q], buf_a.at[h, d], send_a.at[h, d], recv_a.at[h, d], q, g) for d, q in row_peers
        ]

    def second(h):
        return [
            remote(buf_b.at[h, 0], buf_b.at[h, d], send_b.at[h, d], recv_b.at[h, d], r, q) for d, q in grp_peers
        ]

    def third(h):
        return [
            remote(buf_c.at[h, r], buf_c.at[h, r], send_c.at[h, d], recv_c.at[h, d], q, g) for d, q in row_peers
        ]

    def add_rows(h):
        total = buf_x[h, r].astype(F32)
        for (d, _), copy in zip(row_peers, first(h)):
            copy.wait_recv()
            total = total + buf_a[h, d].astype(F32)
        buf_b[h, 0] = total.astype(BF16)
        for copy in second(h):
            copy.start()

    def add_groups(h):
        total = buf_b[h, 0].astype(F32)
        for (d, _), copy in zip(grp_peers, second(h)):
            copy.wait_recv()
            total = total + buf_b[h, d].astype(F32)
        buf_c[h, r] = total.astype(BF16)
        for copy in third(h):
            copy.start()

    def take_rows(h):
        for copy in third(h):
            copy.wait_recv()
        for k in range(R):
            picked[k * c : (k + 1) * c, :] = buf_c[h, k].astype(F32)
        rows_t[h * kh : (h + 1) * kh, :] = picked[...].T.astype(BF16)
        if h == 0:
            for at in parts:
                begun[at, :] = jnp.dot(prev_v[0, at, :kh], rows_t[:kh, :], preferred_element_type=F32)

    square = (256, 256)
    eye = jnp.where(
        lax.broadcasted_iota(jnp.int32, square, 0) == lax.broadcasted_iota(jnp.int32, square, 1), 1.0, 0.0
    ).astype(BF16)
    wide = orb_v.shape[1] // 256

    def turn_orbitals(first, last):
        @pl.loop(first, last)
        def _(i):
            at = pl.ds(pl.multiple_of(i * 256, 256), 256)
            for q in range(wide):
                orb_t[q * 256 : (q + 1) * 256, at] = lax.dot_general(
                    eye, orb_v[at, q * 256 : (q + 1) * 256], (((1,), (1,)), ((), ())), preferred_element_type=F32
                ).astype(BF16)

    tiles = nu // 256
    cuts = [tiles * k // (2 * halves) for k in range(2 * halves + 1)]
    for h in range(halves):
        pick(h)
        if h == 0:
            load_orb.start()
            for mu in range(mu_dev):
                load_pc(mu).start()
            pl.semaphore_wait(barrier, greetings)
        for copy in first(h):
            copy.start()
    load_inv.wait()
    low = lax.broadcasted_iota(jnp.int32, (p, p), 0)
    high = lax.broadcasted_iota(jnp.int32, (p, p), 1)
    upper_v[...] = jnp.where(low <= high, inv_v[...].astype(F32), 0.0).astype(BF16)
    for h in range(halves):
        add_rows(h)
        if h == 0:
            load_orb.wait()
        turn_orbitals(cuts[h], cuts[h + 1])
    for h in range(halves):
        add_groups(h)
        turn_orbitals(cuts[halves + h], cuts[halves + h + 1])
    chunk = nu // 2
    parts = [pl.ds(i * chunk, chunk) for i in range(nu // chunk)]
    for h in range(halves):
        take_rows(h)

    orders = group_orders(G)
    first_mu = 0

    def make_vectors(mu):
        load_pc(mu).wait()
        left = []
        for at in parts:
            if mu is first_mu:
                correction = begun[at, :] + jnp.dot(prev_v[mu, at, kh:], rows_t[kh:, :], preferred_element_type=F32)
            else:
                correction = jnp.dot(prev_v[mu, at, :], rows_t[...], preferred_element_type=F32)
            left.append((new_v[mu, at, :].astype(F32) - correction).astype(BF16))
        for at, residual in zip(parts, left):
            new_v[mu, at, :] = jnp.dot(residual, upper_v[...], preferred_element_type=F32).astype(BF16)

    def add(buf, slot, sem, mu):
        here = buf.at[slot, mu]
        pltpu.make_async_copy(here, here, sem.at[slot, mu]).wait()
        block_v[...] += buf[slot, mu].astype(F32)

    def hand_out(mu, src, dst, send, recv, grp):
        for k in range(R):
            peer = lax.rem(r + k, R)
            remote(src.at[peer], dst.at[r * mu_dev + mu], send, recv, peer, grp).start()

    at_low = g == 0
    at_high = g == G - 1
    at_end = (at_low | at_high) & chained(G)

    def emit(to, mu):
        own = to == g
        if chained(G):
            pl.when(jnp.logical_not(at_low) & ((to > g) | (own & at_high)))(lambda: add(in_up, to, up_sem, mu))
            pl.when(jnp.logical_not(at_high) & ((to < g) | (own & at_low)))(lambda: add(in_down, to, down_sem, mu))
            near = ((to == g + 1) & (to < G - 1)) | ((to == g - 1) & (to > 0))
        else:
            near = jnp.logical_not(own)

        @pl.when(own & jnp.logical_not(at_end))
        def _():
            whole = block_v[...].T
            for k in range(R):
                own_out[mu, k] = whole[k * c : (k + 1) * c, :]
            own_in[r * mu_dev + mu] = own_out[mu, r]
            for k in range(1, R):
                peer = lax.rem(r + k, R)
                remote(own_out.at[mu, peer], own_in.at[r * mu_dev + mu], own_send, own_recv, peer, g).start()

        def turn_last(slot):
            turned = block_v[...].T.astype(BF16)
            for k in range(R):
                last[slot, mu, k] = turned[k * c : (k + 1) * c, :]

        @pl.when(near)
        def _():
            if chained(G):
                slot = jnp.where(to > g, 0, 1)
                into = slot
            else:
                slot = to - (to > g).astype(jnp.int32)
                into = g
            turn_last(slot)
            for k in range(R):
                peer = lax.rem(r + k, R)
                remote(
                    last.at[slot, mu, peer], last_in.at[into, r * mu_dev + mu], last_send, last_recv.at[into], peer, to
                ).start()

        if not chained(G):
            return

        @pl.when(own & at_end)
        def _():
            slot = jnp.where(at_low, 1, 0)
            turn_last(slot)
            last_in[0, r * mu_dev + mu] = last[slot, mu, r]
            for k in range(1, R):
                peer = lax.rem(r + k, R)
                remote(
                    last.at[slot, mu, peer], last_in.at[0, r * mu_dev + mu], own_send, last_recv.at[0], peer, g
                ).start()

        @pl.when(jnp.logical_not(own | near))
        def _():
            send[to, mu] = block_v[...].astype(BF16)

            @pl.when(to > g)
            def _():
                remote(send.at[to, mu], in_up.at[to, mu], hop_sem, up_sem.at[to, mu], r, g + 1).start()

            @pl.when(to < g)
            def _():
                remote(send.at[to, mu], in_down.at[to, mu], hop_sem, down_sem.at[to, mu], r, g - 1).start()

    def block(to, mu):
        at = pl.ds(pl.multiple_of(to * j_dev, j_dev), j_dev)
        block_v[...] = jnp.dot(orb_t[at, :], new_v[mu], preferred_element_type=F32)

    initial = choose(g, [order[0] for order in orders])

    make_vectors(first_mu)
    block(initial, first_mu)
    emit(initial, first_mu)

    @pl.loop(1, mu_dev)
    def _(mu):
        make_vectors(mu)
        block(initial, mu)
        emit(initial, mu)

    for s in range(1, G):
        to = choose(g, [order[s] for order in orders])

        @pl.loop(0, mu_dev)
        def _(mu):
            block(to, mu)
            emit(to, mu)

    def take(buf, sem, when):
        pl.when(when)(pltpu.make_async_copy(buf, buf, sem).wait)

    def gather(slot, when):
        take(last_in.at[slot], last_recv.at[slot], when)

        @pl.when(when)
        def _():
            own_in[...] += last_in[slot].astype(F32)

    inner = jnp.logical_not(at_end)
    others = own_in.at[pl.ds(0, (R - 1) * mu_dev)]
    take(others, own_recv, inner)
    if chained(G):
        gather(0, inner & (2 * g >= G))
        gather(1, inner)
        gather(0, inner & (2 * g < G))
        rounded = last_in.at[0, pl.ds(0, (R - 1) * mu_dev)]
        take(rounded, last_recv.at[0], at_end)

        @pl.when(at_end)
        def _():
            out_v[...] = last_in[0]
    else:
        for slot in range(G):
            gather(slot, g != slot)

    @pl.when(inner)
    def _():
        out_v[...] = own_in[...].astype(BF16)

    for h in range(halves):
        for copy in first(h) + second(h) + third(h):
            copy.wait_send()
    take(others, own_send, inner)
    if chained(G):
        take(rounded, own_send, at_end)
        nears = (g + 1 < G - 1).astype(jnp.int32) + (g - 1 > 0).astype(jnp.int32)
        for count in range(3):
            if count:
                take(last.at[pl.ds(0, count)], last_send, nears == count)
            if G - 1 > count:
                take(send.at[pl.ds(0, G - 1 - count)], hop_sem, nears == count)
    else:
        take(last, last_send, inner)


def fused(pivots, columns, previous, inverse, orbitals, R, G):
    mu_dev, nu, p = columns.shape
    k = previous.shape[2]
    c = p // R
    nj = orbitals.shape[1]
    halves = 2
    kh = k // halves
    hbm = pl.BlockSpec(memory_space=pltpu.HBM)
    slots = 2 if chained(G) else G
    relays = G if chained(G) else 1
    blocks = (R * mu_dev, c, nj // G)
    vmem = pl.BlockSpec(memory_space=pltpu.VMEM)
    dma = pltpu.SemaphoreType.DMA
    return pl.pallas_call(
        functools.partial(fused_kernel, R, G),
        out_shape=(
            jax.ShapeDtypeStruct(blocks, BF16),
            jax.ShapeDtypeStruct(columns.shape, BF16),
        ),
        in_specs=[hbm, hbm, hbm, hbm, hbm],
        out_specs=(vmem, vmem),
        scratch_shapes=[
            pltpu.VMEM((1, p), jnp.int32),
            pltpu.VMEM((p, p), BF16),
            pltpu.VMEM((p, 128), jnp.int32),
            pltpu.VMEM((mu_dev, p, nu), BF16),
            pltpu.VMEM((p, kh), F32),
            pltpu.VMEM((halves, R, c, kh), BF16),
            pltpu.VMEM((halves, R, c, kh), BF16),
            pltpu.VMEM((halves, G, c, kh), BF16),
            pltpu.VMEM((halves, R, c, kh), BF16),
            pltpu.VMEM((k, p), BF16),
            pltpu.VMEM((p, p), BF16),
            pltpu.VMEM((mu_dev, nu, k), BF16),
            pltpu.VMEM((nu, nj), BF16),
            pltpu.VMEM((nj, nu), BF16),
            pltpu.VMEM((nj // G, p), F32),
            pltpu.VMEM((nu, p), F32),
            pltpu.VMEM((relays, mu_dev, nj // G, p), BF16),
            pltpu.VMEM((relays, mu_dev, nj // G, p), BF16),
            pltpu.VMEM((relays, mu_dev, nj // G, p), BF16),
            pltpu.VMEM((2 if chained(G) else G - 1, mu_dev, R, c, nj // G), BF16),
            pltpu.VMEM((mu_dev, R, c, nj // G), F32),
            pltpu.VMEM((slots,) + blocks, BF16),
            pltpu.VMEM(blocks, F32),
            dma((halves, R)), dma((halves, R)), dma((halves, G)), dma((halves, G)), dma((halves, R)), dma((halves, R)),
            dma((2,)), dma((halves, mu_dev)), dma((mu_dev,)), dma(()),
            dma(()), dma((G, mu_dev)), dma((G, mu_dev)), dma(()), dma((slots,)), dma(()), dma(()),
        ],
        compiler_params=pltpu.CompilerParams(
            collective_id=0, has_side_effects=True, vmem_limit_bytes=44 * 1024 * 1024
        ),
        name="fused_exchange",
    )(pivots, columns, previous, inverse, orbitals)


def block_kernel(part_ref, slab_ref, made_ref, out_hbm, new_hbm, out_v, part_v, spread_ref, new_sem, out_sem):
    mus, vecs, j = part_ref.shape
    groups, lot, _, _ = out_v.shape
    wide = mus * lot
    store = pltpu.make_async_copy(made_ref, new_hbm, new_sem)
    store.start()
    mu = lax.broadcasted_iota(jnp.int32, (mus, wide), 0)
    col = lax.broadcasted_iota(jnp.int32, (mus, wide), 1)
    repeat = jnp.where(lax.shift_right_logical(col, lot.bit_length() - 1) == mu, 1.0, 0.0).astype(BF16)
    spread_ref[...] = lax.dot_general(
        slab_ref[...], repeat, (((0,), (0,)), ((), ())), preferred_element_type=F32
    ).astype(BF16)
    for k in range(groups):
        part_v[k] = part_ref[:, k * lot : (k + 1) * lot, :].reshape(wide, j)

    def piece(q, k):
        return pltpu.make_async_copy(out_v.at[k, q], out_hbm.at[k, q], out_sem.at[k, q])

    @pl.loop(0, lot)
    def _(q):
        at = lax.broadcasted_iota(jnp.int32, spread_ref.shape, 1) & (lot - 1)
        kept = jnp.where(at == q, spread_ref[...].astype(F32), 0.0).astype(BF16)
        for k in range(groups):
            out_v[k, q] = jnp.dot(kept, part_v[k], preferred_element_type=F32).astype(BF16)
            piece(q, k).start()

    @pl.loop(0, lot)
    def _(q):
        for k in range(groups):
            piece(q, k).wait()
    store.wait()


def orbital_block(part, slab, made):
    mus, vecs, j = part.shape
    i = slab.shape[1]
    lot = 8
    assert vecs % lot == 0
    groups = vecs // lot
    vmem = pl.BlockSpec(memory_space=pltpu.VMEM)
    anywhere = pl.BlockSpec(memory_space=pl.ANY)
    out, new = pl.pallas_call(
        block_kernel,
        out_shape=(
            jax.ShapeDtypeStruct((groups, lot, i, j), BF16),
            jax.ShapeDtypeStruct(made.shape, BF16),
        ),
        in_specs=[vmem, vmem, vmem],
        out_specs=(anywhere, anywhere),
        scratch_shapes=[
            pltpu.VMEM((groups, lot, i, j), BF16),
            pltpu.VMEM((groups, mus * lot, j), BF16),
            pltpu.VMEM((i, mus * lot), BF16),
            pltpu.SemaphoreType.DMA(()),
            pltpu.SemaphoreType.DMA((groups, lot)),
        ],
        compiler_params=pltpu.CompilerParams(vmem_limit_bytes=40 * 1024 * 1024),
        name="orbital_block",
    )(part, slab, made)
    return out.reshape(vecs, i, j), new


def per_device(R, G, pivot_columns, previous, pivots, pivot_inverse, orbitals, slab_orbitals):
    count = pivot_columns.shape[2]
    stay = functools.partial(pltpu.with_memory_space_constraint, memory_space=pltpu.HBM)
    part, made = fused(
        stay(pivots.reshape(1, count)), pivot_columns, previous, stay(pivot_inverse), orbitals, R, G
    )
    mo_block, new_vectors = orbital_block(part, slab_orbitals, made)
    return new_vectors, mo_block


def solution(mesh):
    R, G = mesh.shape["rows"], mesh.shape["grp"]
    in_specs = (P("rows", "grp", None), P("rows", "grp", None), P(), P(), P("grp", None), P())
    out_specs = (P("rows", "grp", None), P("rows", None, "grp"))
    return jax.shard_map(
        functools.partial(per_device, R, G), mesh=mesh, in_specs=in_specs, out_specs=out_specs,
        check_vma=False,
    )
```

```python
import functools

import jax
import jax.numpy as jnp
from jax import lax
from jax.experimental import pallas as pl
from jax.experimental.pallas import tpu as pltpu
from jax.sharding import PartitionSpec as P

F32 = jnp.float32
BF16 = jnp.bfloat16
MESH = pl.DeviceIdType.MESH


def chained(G):
    return G <= 4


def group_orders(G):
    def due(g, d):
        if d == g:
            return 4 * G if chained(G) and g in (0, G - 1) else -1
        return 2 * (G - 1 - d) + g if d > g else 2 * d + G - 1 - g

    return [sorted(range(G), key=lambda d: (due(g, d), d)) for g in range(G)]


def choose(g, values):
    chosen = jnp.int32(values[0])
    for k in range(1, len(values)):
        chosen = jnp.where(g == k, values[k], chosen)
    return chosen


def fused_kernel(
    R, G, piv_hbm, pc_hbm, prev_hbm, inv_hbm, orb_hbm, out_v, new_v,
    piv_v, inv_v, piv_col, hot_v, picked, buf_x, buf_a, buf_b, buf_c, rows_t, upper_v, prev_v, orb_v, orb_t,
    block_v, begun, send, relay_in, last, own_out, last_in, own_in,
    rows_send, recv_a, recv_b, recv_c, small_sem, prev_sem, pc_sem, orb_sem,
    hop_sem, relay_sem, last_send, last_recv, own_send, own_recv,
):
    r = lax.axis_index("rows")
    g = lax.axis_index("grp")
    mu_dev, nu, p = new_v.shape
    _, _, j_dev, _ = send.shape
    _, c, k_all = buf_c.shape
    halves = 2
    kh = k_all // halves

    load_piv = pltpu.make_async_copy(piv_hbm, piv_v, small_sem.at[0])
    load_inv = pltpu.make_async_copy(inv_hbm, inv_v, small_sem.at[1])
    load_orb = pltpu.make_async_copy(orb_hbm, orb_v, orb_sem)

    def load_prev(h, mu):
        at = pl.ds(h * kh, kh)
        return pltpu.make_async_copy(prev_hbm.at[mu, :, at], prev_v.at[mu, :, at], prev_sem.at[h, mu])

    def load_pc(mu):
        return pltpu.make_async_copy(pc_hbm.at[mu], new_v.at[mu], pc_sem.at[mu])

    load_piv.start()
    barrier = pltpu.get_barrier_semaphore()

    def greet(row, grp):
        pl.semaphore_signal(barrier, inc=1, device_id={"rows": row, "grp": grp}, device_id_type=MESH)

    def greet_rows(step):
        @pl.loop(1, R)
        def _(d):
            greet(lax.rem(r + d, R), lax.rem(g + step + G, G))

    greet_rows(0)
    for d in range(1, G):
        greet(r, lax.rem(g + d, G))
    if chained(G):
        if G > 1:
            pl.when(g > 0)(lambda: greet_rows(-1))
            pl.when(g < G - 1)(lambda: greet_rows(1))
        sides = (g > 0).astype(jnp.int32) + (g < G - 1).astype(jnp.int32)
    else:
        for d in range(1, G):
            greet_rows(d)
        sides = G - 1
    greetings = (sides + 1) * (R - 1) + G - 1
    for h in range(halves):
        for mu in range(mu_dev):
            load_prev(h, mu).start()
    load_inv.start()
    load_piv.wait()

    lanes = piv_col.shape[1]
    piv_col[...] = jnp.broadcast_to(piv_v[...], (lanes, p)).T

    def heat(mu):
        base = (r * mu_dev + mu) * (nu * G) + g * nu
        for i in range(nu // lanes):
            at = lax.broadcasted_iota(jnp.int32, (p, lanes), 1) + (base + i * lanes)
            hot_v[mu, :, i * lanes : (i + 1) * lanes] = jnp.where(piv_col[...] == at, 1.0, 0.0).astype(BF16)

    def remote(src, dst, send, recv, row, grp):
        return pltpu.make_async_remote_copy(
            src_ref=src, dst_ref=dst, send_sem=send, recv_sem=recv,
            device_id={"rows": row, "grp": grp}, device_id_type=MESH,
        )

    row_peers = [(d, lax.rem(r + d, R)) for d in range(1, R)]
    grp_peers = [(d, lax.rem(g + d, G)) for d in range(1, G)]

    pl.loop(0, mu_dev)(heat)

    def pick(h):
        picked[...] = jnp.zeros(picked.shape, F32)

        @pl.loop(0, mu_dev)
        def _(mu):
            load_prev(h, mu).wait()
            picked[...] += jnp.dot(hot_v[mu], prev_v[mu, :, h * kh : (h + 1) * kh], preferred_element_type=F32)

        for k in range(R):
            buf_x[k, :, h * kh : (h + 1) * kh] = picked[k * c : (k + 1) * c, :].astype(BF16)

    def first(cols, n):
        return [
            remote(buf_x.at[q, :, cols], buf_a.at[d, :, cols], rows_send, recv_a.at[n], q, g) for d, q in row_peers
        ]

    def second(cols, n):
        return [
            remote(buf_b.at[0, :, cols], buf_b.at[d, :, cols], rows_send, recv_b.at[n], r, q) for d, q in grp_peers
        ]

    def third(cols, n):
        return [
            remote(buf_c.at[r, :, cols], buf_c.at[r, :, cols], rows_send, recv_c.at[n], q, g) for d, q in row_peers
        ]

    def wait_all(buf, count, cols, sem):
        if count:
            received = buf.at[pl.ds(0, count), :, cols]
            pltpu.make_async_copy(received, received, sem).wait()

    def add_rows(cols, n):
        total = buf_x[r, :, cols].astype(F32)
        wait_all(buf_a, R - 1, cols, recv_a.at[n])
        for d, _ in row_peers:
            total = total + buf_a[d, :, cols].astype(F32)
        buf_b[0, :, cols] = total.astype(BF16)
        for copy in second(cols, n):
            copy.start()

    def add_groups(cols, n):
        total = buf_b[0, :, cols].astype(F32)
        wait_all(buf_b, G - 1, cols, recv_b.at[n])
        for d, _ in grp_peers:
            total = total + buf_b[d, :, cols].astype(F32)
        buf_c[r, :, cols] = total.astype(BF16)
        for copy in third(cols, n):
            copy.start()

    def take_rows(cols, n):
        wait_all(buf_c, R - 1, cols, recv_c.at[n])
        rows_t[cols, :] = buf_c[:, :, cols].reshape(p, cols.size).astype(F32).T.astype(BF16)
        if n == 0:
            for at in parts:
                begun[at, :] = jnp.dot(prev_v[0, at, cols], rows_t[cols, :], preferred_element_type=F32)

    square = (256, 256)
    eye = jnp.where(
        lax.broadcasted_iota(jnp.int32, square, 0) == lax.broadcasted_iota(jnp.int32, square, 1), 1.0, 0.0
    ).astype(BF16)
    wide = orb_v.shape[1] // 256

    def turn_orbitals(first, last):
        @pl.loop(first, last)
        def _(i):
            at = pl.ds(pl.multiple_of(i * 256, 256), 256)
            for q in range(wide):
                orb_t[q * 256 : (q + 1) * 256, at] = lax.dot_general(
                    eye, orb_v[at, q * 256 : (q + 1) * 256], (((1,), (1,)), ((), ())), preferred_element_type=F32
                ).astype(BF16)

    parted = kh // 2 if kh % 256 == 0 else kh
    pieces = [pl.ds(0, kh)] + [pl.ds(kh + at, parted) for at in range(0, kh, parted)]
    tiles = nu // 256
    cuts = [0, tiles // 2, tiles * 4 // 5, tiles]
    for h in range(halves):
        pick(h)
        if h == 0:
            load_orb.start()
            for mu in range(mu_dev):
                load_pc(mu).start()
            pl.semaphore_wait(barrier, greetings)
        for n, cols in enumerate(pieces):
            if (n > 0) == (h > 0):
                for copy in first(cols, n):
                    copy.start()
    load_inv.wait()
    low = lax.broadcasted_iota(jnp.int32, (p, p), 0)
    high = lax.broadcasted_iota(jnp.int32, (p, p), 1)
    upper_v[...] = jnp.where(low <= high, inv_v[...].astype(F32), 0.0).astype(BF16)
    for n, cols in enumerate(pieces):
        add_rows(cols, n)
        if n == 0:
            load_orb.wait()
            turn_orbitals(cuts[0], cuts[1])
    turn_orbitals(cuts[1], cuts[2])
    for n, cols in enumerate(pieces):
        add_groups(cols, n)
        if n == 0:
            turn_orbitals(cuts[2], cuts[3])

    chunk = nu // 2
    parts = [pl.ds(i * chunk, chunk) for i in range(nu // chunk)]
    for n, cols in enumerate(pieces):
        take_rows(cols, n)

    orders = group_orders(G)
    first_mu = 0

    def make_vectors(mu):
        load_pc(mu).wait()
        left = []
        for at in parts:
            if mu is first_mu:
                correction = begun[at, :] + jnp.dot(prev_v[mu, at, kh:], rows_t[kh:, :], preferred_element_type=F32)
            else:
                correction = jnp.dot(prev_v[mu, at, :], rows_t[...], preferred_element_type=F32)
            left.append((new_v[mu, at, :].astype(F32) - correction).astype(BF16))
        for at, residual in zip(parts, left):
            new_v[mu, at, :] = jnp.dot(residual, upper_v[...], preferred_element_type=F32).astype(BF16)

    def add(slot, mu):
        here = relay_in.at[slot, mu]
        pltpu.make_async_copy(here, here, relay_sem.at[slot, mu]).wait()
        block_v[...] += relay_in[slot, mu].astype(F32)

    if R & (R - 1) == 0:
        bits = [1 << b for b in range(R.bit_length() - 1)]
        flips = [(b, b - 2 * b * lax.rem(r // b, 2)) for b in bits]
        everyone = [r + sum(change for b, change in flips if m & b) for m in range(R - 1, -1, -1)]
    else:
        everyone = [lax.rem(r + k, R) for k in range(R - 1, -1, -1)]

    at_low = g == 0
    at_high = g == G - 1
    at_end = (at_low | at_high) & chained(G)

    def emit(to, mu):
        own = to == g
        if chained(G):
            from_low = jnp.logical_not(at_low) & ((to > g) | (own & at_high))
            from_high = jnp.logical_not(at_high) & ((to < g) | (own & at_low))
            pl.when(from_low | from_high)(lambda: add(to, mu))
            near = ((to == g + 1) & (to < G - 1)) | ((to == g - 1) & (to > 0))
        else:
            near = jnp.logical_not(own)

        @pl.when(own & jnp.logical_not(at_end))
        def _():
            whole = block_v[...].T
            for k in range(R):
                own_out[mu, k] = whole[k * c : (k + 1) * c, :]
            own_in[r * mu_dev + mu] = own_out[mu, r]
            for peer in everyone[:-1]:
                remote(own_out.at[mu, peer], own_in.at[r * mu_dev + mu], own_send, own_recv, peer, g).start()

        def turn_last(slot):
            turned = block_v[...].T.astype(BF16)
            for k in range(R):
                last[slot, mu, k] = turned[k * c : (k + 1) * c, :]

        @pl.when(near)
        def _():
            if chained(G):
                slot = jnp.where(to > g, 0, 1)
                into = slot
            else:
                slot = to - (to > g).astype(jnp.int32)
                into = g
            turn_last(slot)
            for peer in everyone:
                remote(
                    last.at[slot, mu, peer], last_in.at[into, r * mu_dev + mu], last_send, last_recv.at[into], peer, to
                ).start()

        if not chained(G):
            return

        @pl.when(own & at_end)
        def _():
            slot = jnp.where(at_low, 1, 0)
            turn_last(slot)
            last_in[0, r * mu_dev + mu] = last[slot, mu, r]
            for peer in everyone[:-1]:
                remote(
                    last.at[slot, mu, peer], last_in.at[0, r * mu_dev + mu], own_send, last_recv.at[0], peer, g
                ).start()

        @pl.when(jnp.logical_not(own | near))
        def _():
            send[to, mu] = block_v[...].astype(BF16)

            via = jnp.where(to > g, g + 1, g - 1)
            remote(send.at[to, mu], relay_in.at[to, mu], hop_sem, relay_sem.at[to, mu], r, via).start()

    def block(to, mu):
        at = pl.ds(pl.multiple_of(to * j_dev, j_dev), j_dev)
        block_v[...] = jnp.dot(orb_t[at, :], new_v[mu], preferred_element_type=F32)

    initial = choose(g, [order[0] for order in orders])

    make_vectors(first_mu)
    block(initial, first_mu)
    emit(initial, first_mu)

    @pl.loop(1, mu_dev)
    def _(mu):
        make_vectors(mu)
        block(initial, mu)
        emit(initial, mu)

    for s in range(1, G):
        to = choose(g, [order[s] for order in orders])

        @pl.loop(0, mu_dev)
        def _(mu):
            block(to, mu)
            emit(to, mu)

    def take(buf, sem, when):
        pl.when(when)(pltpu.make_async_copy(buf, buf, sem).wait)

    def gather(slot, when):
        take(last_in.at[slot], last_recv.at[slot], when)

        @pl.when(when)
        def _():
            own_in[...] += last_in[slot].astype(F32)

    inner = jnp.logical_not(at_end)
    others = own_in.at[pl.ds(0, (R - 1) * mu_dev)]
    take(others, own_recv, inner)
    if chained(G):
        gather(0, inner & (2 * g >= G))
        gather(1, inner)
        gather(0, inner & (2 * g < G))
        rounded = last_in.at[0, pl.ds(0, (R - 1) * mu_dev)]
        take(rounded, last_recv.at[0], at_end)

        @pl.when(at_end)
        def _():
            out_v[...] = last_in[0]
    else:
        for slot in range(G):
            gather(slot, g != slot)

    @pl.when(inner)
    def _():
        out_v[...] = own_in[...].astype(BF16)

    every = pl.ds(0, k_all)
    wait_all(buf_a, R - 1, every, rows_send)
    wait_all(buf_b, G - 1, every, rows_send)
    wait_all(buf_c, R - 1, every, rows_send)
    take(others, own_send, inner)
    if chained(G):
        take(rounded, own_send, at_end)
        nears = (g + 1 < G - 1).astype(jnp.int32) + (g - 1 > 0).astype(jnp.int32)
        for count in range(3):
            if count:
                take(last.at[pl.ds(0, count)], last_send, nears == count)
            if G - 1 > count:
                take(send.at[pl.ds(0, G - 1 - count)], hop_sem, nears == count)
    else:
        take(last, last_send, inner)


def fused(pivots, columns, previous, inverse, orbitals, R, G):
    mu_dev, nu, p = columns.shape
    k = previous.shape[2]
    c = p // R
    nj = orbitals.shape[1]
    halves = 2
    kh = k // halves
    hbm = pl.BlockSpec(memory_space=pltpu.HBM)
    slots = 2 if chained(G) else G
    relays = G if chained(G) else 1
    blocks = (R * mu_dev, c, nj // G)
    vmem = pl.BlockSpec(memory_space=pltpu.VMEM)
    dma = pltpu.SemaphoreType.DMA
    return pl.pallas_call(
        functools.partial(fused_kernel, R, G),
        out_shape=(
            jax.ShapeDtypeStruct(blocks, BF16),
            jax.ShapeDtypeStruct(columns.shape, BF16),
        ),
        in_specs=[hbm, hbm, hbm, hbm, hbm],
        out_specs=(vmem, vmem),
        scratch_shapes=[
            pltpu.VMEM((1, p), jnp.int32),
            pltpu.VMEM((p, p), BF16),
            pltpu.VMEM((p, 128), jnp.int32),
            pltpu.VMEM((mu_dev, p, nu), BF16),
            pltpu.VMEM((p, kh), F32),
            pltpu.VMEM((R, c, k), BF16),
            pltpu.VMEM((R, c, k), BF16),
            pltpu.VMEM((G, c, k), BF16),
            pltpu.VMEM((R, c, k), BF16),
            pltpu.VMEM((k, p), BF16),
            pltpu.VMEM((p, p), BF16),
            pltpu.VMEM((mu_dev, nu, k), BF16),
            pltpu.VMEM((nu, nj), BF16),
            pltpu.VMEM((nj, nu), BF16),
            pltpu.VMEM((nj // G, p), F32),
            pltpu.VMEM((nu, p), F32),
            pltpu.VMEM((relays, mu_dev, nj // G, p), BF16),
            pltpu.VMEM((relays, mu_dev, nj // G, p), BF16),
            pltpu.VMEM((2 if chained(G) else G - 1, mu_dev, R, c, nj // G), BF16),
            pltpu.VMEM((mu_dev, R, c, nj // G), F32),
            pltpu.VMEM((slots,) + blocks, BF16),
            pltpu.VMEM(blocks, F32),
            dma(()), dma((halves + 1,)), dma((halves + 1,)), dma((halves + 1,)), dma((2,)), dma((halves, mu_dev)), dma((mu_dev,)), dma(()),
            dma(()), dma((relays, mu_dev)), dma(()), dma((slots,)), dma(()), dma(()),
        ],
        compiler_params=pltpu.CompilerParams(
            collective_id=0, has_side_effects=True, vmem_limit_bytes=44 * 1024 * 1024
        ),
        name="fused_exchange",
    )(pivots, columns, previous, inverse, orbitals)


def block_kernel(part_ref, slab_ref, made_ref, out_hbm, new_hbm, out_v, part_v, spread_ref, new_sem, out_sem):
    mus, vecs, j = part_ref.shape
    groups, lot, _, _ = out_v.shape
    wide = mus * lot
    store = pltpu.make_async_copy(made_ref, new_hbm, new_sem)
    store.start()
    mu = lax.broadcasted_iota(jnp.int32, (mus, wide), 0)
    col = lax.broadcasted_iota(jnp.int32, (mus, wide), 1)
    repeat = jnp.where(lax.shift_right_logical(col, lot.bit_length() - 1) == mu, 1.0, 0.0).astype(BF16)
    spread_ref[...] = lax.dot_general(
        slab_ref[...], repeat, (((0,), (0,)), ((), ())), preferred_element_type=F32
    ).astype(BF16)
    for k in range(groups):
        part_v[k] = part_ref[:, k * lot : (k + 1) * lot, :].reshape(wide, j)

    def piece(q, k):
        return pltpu.make_async_copy(out_v.at[k, q], out_hbm.at[k, q], out_sem)

    @pl.loop(0, lot)
    def _(q):
        at = lax.broadcasted_iota(jnp.int32, spread_ref.shape, 1) & (lot - 1)
        kept = jnp.where(at == q, spread_ref[...].astype(F32), 0.0).astype(BF16)
        for k in range(groups):
            out_v[k, q] = jnp.dot(kept, part_v[k], preferred_element_type=F32).astype(BF16)
            piece(q, k).start()

    pltpu.make_async_copy(out_v, out_hbm, out_sem).wait()
    store.wait()


def orbital_block(part, slab, made):
    mus, vecs, j = part.shape
    i = slab.shape[1]
    lot = 8
    assert vecs % lot == 0
    groups = vecs // lot
    vmem = pl.BlockSpec(memory_space=pltpu.VMEM)
    anywhere = pl.BlockSpec(memory_space=pl.ANY)
    out, new = pl.pallas_call(
        block_kernel,
        out_shape=(
            jax.ShapeDtypeStruct((groups, lot, i, j), BF16),
            jax.ShapeDtypeStruct(made.shape, BF16),
        ),
        in_specs=[vmem, vmem, vmem],
        out_specs=(anywhere, anywhere),
        scratch_shapes=[
            pltpu.VMEM((groups, lot, i, j), BF16),
            pltpu.VMEM((groups, mus * lot, j), BF16),
            pltpu.VMEM((i, mus * lot), BF16),
            pltpu.SemaphoreType.DMA(()),
            pltpu.SemaphoreType.DMA(()),
        ],
        compiler_params=pltpu.CompilerParams(vmem_limit_bytes=40 * 1024 * 1024),
        name="orbital_block",
    )(part, slab, made)
    return out.reshape(vecs, i, j), new


def per_device(R, G, pivot_columns, previous, pivots, pivot_inverse, orbitals, slab_orbitals):
    count = pivot_columns.shape[2]
    stay = functools.partial(pltpu.with_memory_space_constraint, memory_space=pltpu.HBM)
    part, made = fused(
        stay(pivots.reshape(1, count)), pivot_columns, previous, stay(pivot_inverse), orbitals, R, G
    )
    mo_block, new_vectors = orbital_block(part, slab_orbitals, made)
    return new_vectors, mo_block


def solution(mesh):
    R, G = mesh.shape["rows"], mesh.shape["grp"]
    in_specs = (P("rows", "grp", None), P("rows", "grp", None), P(), P(), P("grp", None), P())
    out_specs = (P("rows", "grp", None), P("rows", None, "grp"))
    return jax.shard_map(
        functools.partial(per_device, R, G), mesh=mesh, in_specs=in_specs, out_specs=out_specs,
        check_vma=False,
    )
```

```python
import functools

import jax
import jax.numpy as jnp
from jax import lax
from jax.experimental import pallas as pl
from jax.experimental.pallas import tpu as pltpu
from jax.sharding import PartitionSpec as P

F32 = jnp.float32
BF16 = jnp.bfloat16
MESH = pl.DeviceIdType.MESH


def chained(G):
    return G <= 4


def group_orders(G):
    def due(g, d):
        if d == g:
            return 4 * G if chained(G) and g in (0, G - 1) else -1
        return 2 * (G - 1 - d) + g if d > g else 2 * d + G - 1 - g

    return [sorted(range(G), key=lambda d: (due(g, d), d)) for g in range(G)]


def choose(g, values):
    chosen = jnp.int32(values[0])
    for k in range(1, len(values)):
        chosen = jnp.where(g == k, values[k], chosen)
    return chosen


def fused_kernel(
    R, G, piv_hbm, pc_hbm, prev_hbm, inv_hbm, orb_hbm, out_v, new_v,
    piv_v, inv_v, piv_col, hot_v, picked, buf_x, buf_a, buf_b, buf_c, rows_t, upper_v, prev_v, orb_v, orb_t,
    block_v, begun, send, relay_in, last, own_out, last_in, own_in,
    rows_send, recv_a, recv_b, recv_c, small_sem, prev_sem, pc_sem, orb_sem,
    hop_sem, relay_sem, last_send, last_recv, own_send, own_recv,
):
    r = lax.axis_index("rows")
    g = lax.axis_index("grp")
    mu_dev, nu, p = new_v.shape
    _, _, j_dev, _ = send.shape
    _, c, k_all = buf_c.shape
    halves = 2
    kh = k_all // halves

    load_piv = pltpu.make_async_copy(piv_hbm, piv_v, small_sem.at[0])
    load_inv = pltpu.make_async_copy(inv_hbm, inv_v, small_sem.at[1])
    load_orb = pltpu.make_async_copy(orb_hbm, orb_v, orb_sem)

    def load_prev(h, mu):
        at = pl.ds(h * kh, kh)
        return pltpu.make_async_copy(prev_hbm.at[mu, :, at], prev_v.at[mu, :, at], prev_sem.at[h, mu])

    def load_pc(mu):
        return pltpu.make_async_copy(pc_hbm.at[mu], new_v.at[mu], pc_sem.at[mu])

    load_piv.start()
    barrier = pltpu.get_barrier_semaphore()

    def greet(row, grp):
        pl.semaphore_signal(barrier, inc=1, device_id={"rows": row, "grp": grp}, device_id_type=MESH)

    def greet_rows(step):
        @pl.loop(1, R)
        def _(d):
            greet(lax.rem(r + d, R), lax.rem(g + step + G, G))

    greet_rows(0)
    for d in range(1, G):
        greet(r, lax.rem(g + d, G))
    if chained(G):
        if G > 1:
            pl.when(g > 0)(lambda: greet_rows(-1))
            pl.when(g < G - 1)(lambda: greet_rows(1))
        sides = (g > 0).astype(jnp.int32) + (g < G - 1).astype(jnp.int32)
    else:
        for d in range(1, G):
            greet_rows(d)
        sides = G - 1
    greetings = (sides + 1) * (R - 1) + G - 1
    for h in range(halves):
        for mu in range(mu_dev):
            load_prev(h, mu).start()
    load_inv.start()
    load_piv.wait()

    lanes = piv_col.shape[1]
    piv_col[...] = jnp.broadcast_to(piv_v[...], (lanes, p)).T

    def heat(mu):
        base = (r * mu_dev + mu) * (nu * G) + g * nu
        for i in range(nu // lanes):
            at = lax.broadcasted_iota(jnp.int32, (p, lanes), 1) + (base + i * lanes)
            hot_v[mu, :, i * lanes : (i + 1) * lanes] = jnp.where(piv_col[...] == at, 1.0, 0.0).astype(BF16)

    def remote(src, dst, send, recv, row, grp):
        return pltpu.make_async_remote_copy(
            src_ref=src, dst_ref=dst, send_sem=send, recv_sem=recv,
            device_id={"rows": row, "grp": grp}, device_id_type=MESH,
        )

    if R & (R - 1) == 0:
        bits = [1 << b for b in range(R.bit_length() - 1)]
        flips = [(b, b - 2 * b * lax.rem(r // b, 2)) for b in bits]
        everyone = [r + sum(change for b, change in flips if m & b) for m in range(R - 1, -1, -1)]
        row_peers = [(R - 1 - k, q) for k, q in enumerate(everyone[:-1])]
    else:
        everyone = [lax.rem(r + k, R) for k in range(R - 1, -1, -1)]
        row_peers = [(R - 1 - k, q) for k, q in enumerate(everyone[:-1])]

    turns = [jnp.where(2 * g < G, G - d, d) for d in range(1, G)]
    grp_peers = [(d, lax.rem(g + d, G)) for d in turns]

    pl.loop(0, mu_dev)(heat)

    def pick(h):
        picked[...] = jnp.zeros(picked.shape, F32)

        @pl.loop(0, mu_dev)
        def _(mu):
            load_prev(h, mu).wait()
            picked[...] += jnp.dot(hot_v[mu], prev_v[mu, :, h * kh : (h + 1) * kh], preferred_element_type=F32)

        for k in range(R):
            buf_x[k, :, h * kh : (h + 1) * kh] = picked[k * c : (k + 1) * c, :].astype(BF16)

    def first(cols, n):
        return [
            remote(buf_x.at[q, :, cols], buf_a.at[d, :, cols], rows_send, recv_a.at[n], q, g) for d, q in row_peers
        ]

    def second(cols, n):
        return [
            remote(buf_b.at[0, :, cols], buf_b.at[d, :, cols], rows_send, recv_b.at[n], r, q) for d, q in grp_peers
        ]

    def third(cols, n):
        return [
            remote(buf_c.at[r, :, cols], buf_c.at[r, :, cols], rows_send, recv_c.at[n], q, g) for d, q in row_peers
        ]

    def wait_all(buf, count, cols, sem):
        if count:
            received = buf.at[pl.ds(0, count), :, cols]
            pltpu.make_async_copy(received, received, sem).wait()

    def add_rows(cols, n):
        total = buf_x[r, :, cols].astype(F32)
        wait_all(buf_a, R - 1, cols, recv_a.at[n])
        for d, _ in row_peers:
            total = total + buf_a[d, :, cols].astype(F32)
        buf_b[0, :, cols] = total.astype(BF16)
        for copy in second(cols, n):
            copy.start()

    def add_groups(cols, n):
        total = buf_b[0, :, cols].astype(F32)
        wait_all(buf_b, G - 1, cols, recv_b.at[n])
        for d, _ in grp_peers:
            total = total + buf_b[d, :, cols].astype(F32)
        buf_c[r, :, cols] = total.astype(BF16)
        for copy in third(cols, n):
            copy.start()

    def take_rows(cols, n):
        wait_all(buf_c, R - 1, cols, recv_c.at[n])
        rows_t[cols, :] = buf_c[:, :, cols].reshape(p, cols.size).astype(F32).T.astype(BF16)
        if n == 0:
            for at in parts:
                begun[at, :] = jnp.dot(prev_v[0, at, cols], rows_t[cols, :], preferred_element_type=F32)

    square = (256, 256)
    eye = jnp.where(
        lax.broadcasted_iota(jnp.int32, square, 0) == lax.broadcasted_iota(jnp.int32, square, 1), 1.0, 0.0
    ).astype(BF16)
    wide = orb_v.shape[1] // 256

    def turn_orbitals(first, last):
        @pl.loop(first, last)
        def _(i):
            at = pl.ds(pl.multiple_of(i * 256, 256), 256)
            for q in range(wide):
                orb_t[q * 256 : (q + 1) * 256, at] = lax.dot_general(
                    eye, orb_v[at, q * 256 : (q + 1) * 256], (((1,), (1,)), ((), ())), preferred_element_type=F32
                ).astype(BF16)

    parted = kh // 2 if kh % 256 == 0 else kh
    pieces = [pl.ds(0, kh)] + [pl.ds(kh + at, parted) for at in range(0, kh, parted)]
    tiles = nu // 256
    cuts = [0, tiles // 2, tiles * 4 // 5, tiles]
    for h in range(halves):
        pick(h)
        if h == 0:
            load_orb.start()
            for mu in range(mu_dev):
                load_pc(mu).start()
            pl.semaphore_wait(barrier, greetings)
        for n, cols in enumerate(pieces):
            if (n > 0) == (h > 0):
                for copy in first(cols, n):
                    copy.start()
    load_inv.wait()
    low = lax.broadcasted_iota(jnp.int32, (p, p), 0)
    high = lax.broadcasted_iota(jnp.int32, (p, p), 1)
    upper_v[...] = jnp.where(low <= high, inv_v[...].astype(F32), 0.0).astype(BF16)
    for n, cols in enumerate(pieces):
        add_rows(cols, n)
        if n == 0:
            load_orb.wait()
            turn_orbitals(cuts[0], cuts[1])
    turn_orbitals(cuts[1], cuts[2])
    for n, cols in enumerate(pieces):
        add_groups(cols, n)
        if n == 0:
            turn_orbitals(cuts[2], cuts[3])

    chunk = nu // 2
    parts = [pl.ds(i * chunk, chunk) for i in range(nu // chunk)]
    for n, cols in enumerate(pieces):
        take_rows(cols, n)

    orders = group_orders(G)
    first_mu = 0

    def make_vectors(mu):
        load_pc(mu).wait()
        left = []
        for at in parts:
            if mu is first_mu:
                correction = begun[at, :] + jnp.dot(prev_v[mu, at, kh:], rows_t[kh:, :], preferred_element_type=F32)
            else:
                correction = jnp.dot(prev_v[mu, at, :], rows_t[...], preferred_element_type=F32)
            left.append((new_v[mu, at, :].astype(F32) - correction).astype(BF16))
        for at, residual in zip(parts, left):
            new_v[mu, at, :] = jnp.dot(residual, upper_v[...], preferred_element_type=F32).astype(BF16)

    def add(slot, mu):
        here = relay_in.at[slot, mu]
        pltpu.make_async_copy(here, here, relay_sem.at[slot, mu]).wait()
        block_v[...] += relay_in[slot, mu].astype(F32)

    at_low = g == 0
    at_high = g == G - 1
    at_end = (at_low | at_high) & chained(G)

    def hop(to, at, sem):
        via = jnp.where(to > g, g + 1, g - 1)
        remote(send.at[at], relay_in.at[at], hop_sem, relay_sem.at[sem], r, via).start()

    def emit(to, mu):
        own = to == g
        if chained(G):
            from_low = jnp.logical_not(at_low) & ((to > g) | (own & at_high))
            from_high = jnp.logical_not(at_high) & ((to < g) | (own & at_low))
            pl.when(from_low | from_high)(lambda: add(to, mu))
            near = ((to == g + 1) & (to < G - 1)) | ((to == g - 1) & (to > 0))
        else:
            near = jnp.logical_not(own)

        @pl.when(own & jnp.logical_not(at_end))
        def _():
            whole = block_v[...].T
            for k in range(R):
                own_out[mu, k] = whole[k * c : (k + 1) * c, :]
            own_in[r * mu_dev + mu] = own_out[mu, r]
            for peer in everyone[:-1]:
                remote(own_out.at[mu, peer], own_in.at[r * mu_dev + mu], own_send, own_recv, peer, g).start()

        def turn_last(slot):
            turned = block_v[...].T.astype(BF16)
            for k in range(R):
                last[slot, mu, k] = turned[k * c : (k + 1) * c, :]

        @pl.when(near)
        def _():
            if chained(G):
                slot = jnp.where(to > g, 0, 1)
                into = slot
            else:
                slot = to - (to > g).astype(jnp.int32)
                into = g
            turn_last(slot)
            for peer in everyone:
                remote(
                    last.at[slot, mu, peer], last_in.at[into, r * mu_dev + mu], last_send, last_recv.at[into], peer, to
                ).start()

        if not chained(G):
            return

        @pl.when(own & at_end)
        def _():
            slot = jnp.where(at_low, 1, 0)
            turn_last(slot)
            last_in[0, r * mu_dev + mu] = last[slot, mu, r]
            for peer in everyone[:-1]:
                remote(
                    last.at[slot, mu, peer], last_in.at[0, r * mu_dev + mu], own_send, last_recv.at[0], peer, g
                ).start()

        @pl.when(jnp.logical_not(own | near))
        def _():
            send[to, mu] = block_v[...].astype(BF16)

            hop(to, (to, mu), (to, mu))

    def block(to, mu):
        at = pl.ds(pl.multiple_of(to * j_dev, j_dev), j_dev)
        block_v[...] = jnp.dot(orb_t[at, :], new_v[mu], preferred_element_type=F32)

    initial = choose(g, [order[0] for order in orders])

    make_vectors(first_mu)
    if chained(G) and G > 1:
        for half in range(2):
            rows = pl.ds(half * (j_dev // 2), j_dev // 2)
            at = pl.ds(pl.multiple_of(initial * j_dev + half * (j_dev // 2), j_dev // 2), j_dev // 2)
            block_v[rows, :] = jnp.dot(orb_t[at, :], new_v[first_mu], preferred_element_type=F32)

            @pl.when(at_end)
            def _():
                send[initial, first_mu, rows, :] = block_v[rows, :].astype(BF16)
                hop(initial, (initial, first_mu, rows), (initial, first_mu))

        pl.when(jnp.logical_not(at_end))(lambda: emit(initial, first_mu))
    else:
        block(initial, first_mu)
        emit(initial, first_mu)

    @pl.loop(1, mu_dev)
    def _(mu):
        make_vectors(mu)
        block(initial, mu)
        emit(initial, mu)

    rest = list(range(1, G))
    paired = rest[-2:] if chained(G) and G > 2 else []
    for s in rest[: len(rest) - len(paired)]:
        to = choose(g, [order[s] for order in orders])

        @pl.loop(0, mu_dev)
        def _(mu):
            block(to, mu)
            emit(to, mu)

    if paired:
        one, two = [choose(g, [order[s] for order in orders]) for s in paired]

        @pl.loop(0, 2 * mu_dev)
        def _(t):
            second_one = jnp.where(at_end, t // mu_dev, lax.rem(t, 2))
            mu = jnp.where(at_end, lax.rem(t, mu_dev), t // 2)
            to = jnp.where(second_one == 0, one, two)
            block(to, mu)
            emit(to, mu)

    def take(buf, sem, when):
        pl.when(when)(pltpu.make_async_copy(buf, buf, sem).wait)

    def gather(slot, when):
        take(last_in.at[slot], last_recv.at[slot], when)

        @pl.when(when)
        def _():
            own_in[...] += last_in[slot].astype(F32)

    inner = jnp.logical_not(at_end)
    others = own_in.at[pl.ds(0, (R - 1) * mu_dev)]
    take(others, own_recv, inner)
    if chained(G):
        gather(0, inner & (2 * g >= G))
        gather(1, inner)
        gather(0, inner & (2 * g < G))
        rounded = last_in.at[0, pl.ds(0, (R - 1) * mu_dev)]
        take(rounded, last_recv.at[0], at_end)

        @pl.when(at_end)
        def _():
            out_v[...] = last_in[0]
    else:
        for slot in range(G):
            gather(slot, g != slot)

    @pl.when(inner)
    def _():
        out_v[...] = own_in[...].astype(BF16)

    every = pl.ds(0, k_all)
    wait_all(buf_a, R - 1, every, rows_send)
    wait_all(buf_b, G - 1, every, rows_send)
    wait_all(buf_c, R - 1, every, rows_send)
    take(others, own_send, inner)
    if chained(G):
        take(rounded, own_send, at_end)
        nears = (g + 1 < G - 1).astype(jnp.int32) + (g - 1 > 0).astype(jnp.int32)
        for count in range(3):
            if count:
                take(last.at[pl.ds(0, count)], last_send, nears == count)
            if G - 1 > count:
                take(send.at[pl.ds(0, G - 1 - count)], hop_sem, nears == count)
    else:
        take(last, last_send, inner)


def fused(pivots, columns, previous, inverse, orbitals, R, G):
    mu_dev, nu, p = columns.shape
    k = previous.shape[2]
    c = p // R
    nj = orbitals.shape[1]
    halves = 2
    kh = k // halves
    hbm = pl.BlockSpec(memory_space=pltpu.HBM)
    slots = 2 if chained(G) else G
    relays = G if chained(G) else 1
    blocks = (R * mu_dev, c, nj // G)
    vmem = pl.BlockSpec(memory_space=pltpu.VMEM)
    dma = pltpu.SemaphoreType.DMA
    return pl.pallas_call(
        functools.partial(fused_kernel, R, G),
        out_shape=(
            jax.ShapeDtypeStruct(blocks, BF16),
            jax.ShapeDtypeStruct(columns.shape, BF16),
        ),
        in_specs=[hbm, hbm, hbm, hbm, hbm],
        out_specs=(vmem, vmem),
        scratch_shapes=[
            pltpu.VMEM((1, p), jnp.int32),
            pltpu.VMEM((p, p), BF16),
            pltpu.VMEM((p, 128), jnp.int32),
            pltpu.VMEM((mu_dev, p, nu), BF16),
            pltpu.VMEM((p, kh), F32),
            pltpu.VMEM((R, c, k), BF16),
            pltpu.VMEM((R, c, k), BF16),
            pltpu.VMEM((G, c, k), BF16),
            pltpu.VMEM((R, c, k), BF16),
            pltpu.VMEM((k, p), BF16),
            pltpu.VMEM((p, p), BF16),
            pltpu.VMEM((mu_dev, nu, k), BF16),
            pltpu.VMEM((nu, nj), BF16),
            pltpu.VMEM((nj, nu), BF16),
            pltpu.VMEM((nj // G, p), F32),
            pltpu.VMEM((nu, p), F32),
            pltpu.VMEM((relays, mu_dev, nj // G, p), BF16),
            pltpu.VMEM((relays, mu_dev, nj // G, p), BF16),
            pltpu.VMEM((2 if chained(G) else G - 1, mu_dev, R, c, nj // G), BF16),
            pltpu.VMEM((mu_dev, R, c, nj // G), F32),
            pltpu.VMEM((slots,) + blocks, BF16),
            pltpu.VMEM(blocks, F32),
            dma(()), dma((halves + 1,)), dma((halves + 1,)), dma((halves + 1,)), dma((2,)), dma((halves, mu_dev)), dma((mu_dev,)), dma(()),
            dma(()), dma((relays, mu_dev)), dma(()), dma((slots,)), dma(()), dma(()),
        ],
        compiler_params=pltpu.CompilerParams(
            collective_id=0, has_side_effects=True, vmem_limit_bytes=44 * 1024 * 1024
        ),
        name="fused_exchange",
    )(pivots, columns, previous, inverse, orbitals)


def block_kernel(part_ref, slab_ref, made_ref, out_hbm, new_hbm, out_v, part_v, spread_ref, new_sem, out_sem):
    mus, vecs, j = part_ref.shape
    groups, lot, _, _ = out_v.shape
    wide = mus * lot
    store = pltpu.make_async_copy(made_ref, new_hbm, new_sem)
    store.start()
    mu = lax.broadcasted_iota(jnp.int32, (mus, wide), 0)
    col = lax.broadcasted_iota(jnp.int32, (mus, wide), 1)
    repeat = jnp.where(lax.shift_right_logical(col, lot.bit_length() - 1) == mu, 1.0, 0.0).astype(BF16)
    spread_ref[...] = lax.dot_general(
        slab_ref[...], repeat, (((0,), (0,)), ((), ())), preferred_element_type=F32
    ).astype(BF16)
    for k in range(groups):
        part_v[k] = part_ref[:, k * lot : (k + 1) * lot, :].reshape(wide, j)

    def piece(q, k):
        return pltpu.make_async_copy(out_v.at[k, q], out_hbm.at[k, q], out_sem)

    @pl.loop(0, lot)
    def _(q):
        at = lax.broadcasted_iota(jnp.int32, spread_ref.shape, 1) & (lot - 1)
        kept = jnp.where(at == q, spread_ref[...].astype(F32), 0.0).astype(BF16)
        for k in range(groups):
            out_v[k, q] = jnp.dot(kept, part_v[k], preferred_element_type=F32).astype(BF16)
            piece(q, k).start()

    pltpu.make_async_copy(out_v, out_hbm, out_sem).wait()
    store.wait()


def orbital_block(part, slab, made):
    mus, vecs, j = part.shape
    i = slab.shape[1]
    lot = 8
    assert vecs % lot == 0
    groups = vecs // lot
    vmem = pl.BlockSpec(memory_space=pltpu.VMEM)
    anywhere = pl.BlockSpec(memory_space=pl.ANY)
    out, new = pl.pallas_call(
        block_kernel,
        out_shape=(
            jax.ShapeDtypeStruct((groups, lot, i, j), BF16),
            jax.ShapeDtypeStruct(made.shape, BF16),
        ),
        in_specs=[vmem, vmem, vmem],
        out_specs=(anywhere, anywhere),
        scratch_shapes=[
            pltpu.VMEM((groups, lot, i, j), BF16),
            pltpu.VMEM((groups, mus * lot, j), BF16),
            pltpu.VMEM((i, mus * lot), BF16),
            pltpu.SemaphoreType.DMA(()),
            pltpu.SemaphoreType.DMA(()),
        ],
        compiler_params=pltpu.CompilerParams(vmem_limit_bytes=40 * 1024 * 1024),
        name="orbital_block",
    )(part, slab, made)
    return out.reshape(vecs, i, j), new


def per_device(R, G, pivot_columns, previous, pivots, pivot_inverse, orbitals, slab_orbitals):
    count = pivot_columns.shape[2]
    stay = functools.partial(pltpu.with_memory_space_constraint, memory_space=pltpu.HBM)
    part, made = fused(
        stay(pivots.reshape(1, count)), pivot_columns, previous, stay(pivot_inverse), orbitals, R, G
    )
    mo_block, new_vectors = orbital_block(part, slab_orbitals, made)
    return new_vectors, mo_block


def solution(mesh):
    R, G = mesh.shape["rows"], mesh.shape["grp"]
    in_specs = (P("rows", "grp", None), P("rows", "grp", None), P(), P(), P("grp", None), P())
    out_specs = (P("rows", "grp", None), P("rows", None, "grp"))
    return jax.shard_map(
        functools.partial(per_device, R, G), mesh=mesh, in_specs=in_specs, out_specs=out_specs,
        check_vma=False,
    )
```

```python
import functools

import jax
import jax.numpy as jnp
from jax import lax
from jax.experimental import pallas as pl
from jax.experimental.pallas import tpu as pltpu
from jax.sharding import PartitionSpec as P

F32 = jnp.float32
BF16 = jnp.bfloat16
MESH = pl.DeviceIdType.MESH


def chained(G):
    return G <= 4


def group_orders(G):
    def due(g, d):
        if d == g:
            return 4 * G if chained(G) and g in (0, G - 1) else -1
        return 2 * (G - 1 - d) + g if d > g else 2 * d + G - 1 - g

    return [sorted(range(G), key=lambda d: (due(g, d), d)) for g in range(G)]


def choose(g, values):
    chosen = jnp.int32(values[0])
    for k in range(1, len(values)):
        chosen = jnp.where(g == k, values[k], chosen)
    return chosen


def fused_kernel(
    R, G, piv_hbm, pc_hbm, prev_hbm, inv_hbm, orb_hbm, out_v, new_v,
    piv_v, inv_v, piv_col, within, hot_v, picked, buf_x, buf_a, buf_b, buf_c, rows_t, upper_v, prev_v, orb_v, orb_t,
    block_v, begun, send, relay_in, last, own_out, last_in, own_in,
    rows_send, recv_a, recv_b, recv_c, small_sem, prev_sem, pc_sem, orb_sem,
    hop_sem, relay_sem, last_send, last_recv, own_send, own_recv,
):
    r = lax.axis_index("rows")
    g = lax.axis_index("grp")
    mu_dev, nu, p = new_v.shape
    _, _, j_dev, _ = send.shape
    _, c, k_all = buf_c.shape
    halves = 2
    kh = k_all // halves

    load_piv = pltpu.make_async_copy(piv_hbm, piv_v, small_sem.at[0])
    load_inv = pltpu.make_async_copy(inv_hbm, inv_v, small_sem.at[1])
    load_orb = pltpu.make_async_copy(orb_hbm, orb_v, orb_sem)

    def load_prev(h, mu):
        at = pl.ds(h * kh, kh)
        return pltpu.make_async_copy(prev_hbm.at[mu, :, at], prev_v.at[mu, :, at], prev_sem.at[h, mu])

    def load_pc(mu):
        return pltpu.make_async_copy(pc_hbm.at[mu], new_v.at[mu], pc_sem.at[mu])

    load_piv.start()
    barrier = pltpu.get_barrier_semaphore()

    def greet(row, grp):
        pl.semaphore_signal(barrier, inc=1, device_id={"rows": row, "grp": grp}, device_id_type=MESH)

    def greet_rows(step):
        @pl.loop(1, R)
        def _(d):
            greet(lax.rem(r + d, R), lax.rem(g + step + G, G))

    greet_rows(0)
    for d in range(1, G):
        greet(r, lax.rem(g + d, G))
    for h in range(halves):
        for mu in range(mu_dev):
            load_prev(h, mu).start()
    if chained(G):
        if G > 1:
            pl.when(g > 0)(lambda: greet_rows(-1))
            pl.when(g < G - 1)(lambda: greet_rows(1))
        sides = (g > 0).astype(jnp.int32) + (g < G - 1).astype(jnp.int32)
    else:
        for d in range(1, G):
            greet_rows(d)
        sides = G - 1
    greetings = (sides + 1) * (R - 1) + G - 1
    load_inv.start()
    load_piv.wait()

    lanes = piv_col.shape[1]
    turned_piv = jnp.broadcast_to(piv_v[...], (lanes, p)).T
    lane = lax.broadcasted_iota(jnp.int32, (p, lanes), 1)
    piv_col[...] = lax.shift_right_arithmetic(turned_piv, lanes.bit_length() - 1)
    within[...] = jnp.where((turned_piv & (lanes - 1)) == lane, 1.0, 0.0).astype(BF16)

    def heat(mu):
        base = (r * mu_dev + mu) * (nu * G) + g * nu
        tile = (piv_col[...] - base // lanes).astype(F32).astype(BF16)
        for i in range(nu // lanes):
            here = tile == jnp.full(tile.shape, i, BF16)
            hot_v[mu, :, i * lanes : (i + 1) * lanes] = jnp.where(here, within[...], jnp.zeros(tile.shape, BF16))

    def remote(src, dst, send, recv, row, grp):
        return pltpu.make_async_remote_copy(
            src_ref=src, dst_ref=dst, send_sem=send, recv_sem=recv,
            device_id={"rows": row, "grp": grp}, device_id_type=MESH,
        )

    if R & (R - 1) == 0:
        bits = [1 << b for b in range(R.bit_length() - 1)]
        flips = [(b, b - 2 * b * lax.rem(r // b, 2)) for b in bits]
        everyone = [r + sum(change for b, change in flips if m & b) for m in range(R - 1, -1, -1)]
        row_peers = [(R - 1 - k, q) for k, q in enumerate(everyone[:-1])]
    else:
        everyone = [lax.rem(r + k, R) for k in range(R - 1, -1, -1)]
        row_peers = [(R - 1 - k, q) for k, q in enumerate(everyone[:-1])]

    turns = [jnp.where(2 * g < G, G - d, d) for d in range(1, G)]
    grp_peers = [(d, lax.rem(g + d, G)) for d in turns]

    pl.loop(0, mu_dev)(heat)

    def pick(h):
        picked[...] = jnp.zeros(picked.shape, F32)

        @pl.loop(0, mu_dev)
        def _(mu):
            load_prev(h, mu).wait()
            picked[...] += jnp.dot(hot_v[mu], prev_v[mu, :, h * kh : (h + 1) * kh], preferred_element_type=F32)

        for k in range(R):
            buf_x[k, :, h * kh : (h + 1) * kh] = picked[k * c : (k + 1) * c, :].astype(BF16)

    def first(cols, n):
        return [
            remote(buf_x.at[q, :, cols], buf_a.at[d, :, cols], rows_send, recv_a.at[n], q, g) for d, q in row_peers
        ]

    def second(cols, n):
        return [
            remote(buf_b.at[0, :, cols], buf_b.at[d, :, cols], rows_send, recv_b.at[n], r, q) for d, q in grp_peers
        ]

    def third(cols, n):
        return [
            remote(buf_c.at[r, :, cols], buf_c.at[r, :, cols], rows_send, recv_c.at[n], q, g) for d, q in row_peers
        ]

    def wait_all(buf, count, cols, sem):
        if count:
            received = buf.at[pl.ds(0, count), :, cols]
            pltpu.make_async_copy(received, received, sem).wait()

    def add_rows(cols, n):
        total = buf_x[r, :, cols].astype(F32)
        wait_all(buf_a, R - 1, cols, recv_a.at[n])
        for d, _ in row_peers:
            total = total + buf_a[d, :, cols].astype(F32)
        buf_b[0, :, cols] = total.astype(BF16)
        for copy in second(cols, n):
            copy.start()

    def add_groups(cols, n):
        total = buf_b[0, :, cols].astype(F32)
        wait_all(buf_b, G - 1, cols, recv_b.at[n])
        for d, _ in grp_peers:
            total = total + buf_b[d, :, cols].astype(F32)
        buf_c[r, :, cols] = total.astype(BF16)
        for copy in third(cols, n):
            copy.start()

    def take_rows(cols, n):
        wait_all(buf_c, R - 1, cols, recv_c.at[n])
        rows_t[cols, :] = buf_c[:, :, cols].reshape(p, cols.size).astype(F32).T.astype(BF16)
        if n == 0:
            for at in parts:
                begun[at, :] = jnp.dot(prev_v[0, at, cols], rows_t[cols, :], preferred_element_type=F32)

    square = (256, 256)
    eye = jnp.where(
        lax.broadcasted_iota(jnp.int32, square, 0) == lax.broadcasted_iota(jnp.int32, square, 1), 1.0, 0.0
    ).astype(BF16)
    wide = orb_v.shape[1] // 256

    def turn_orbitals(first, last):
        @pl.loop(first, last)
        def _(i):
            at = pl.ds(pl.multiple_of(i * 256, 256), 256)
            for q in range(wide):
                orb_t[q * 256 : (q + 1) * 256, at] = lax.dot_general(
                    eye, orb_v[at, q * 256 : (q + 1) * 256], (((1,), (1,)), ((), ())), preferred_element_type=F32
                ).astype(BF16)

    parted = kh // 2 if kh % 256 == 0 else kh
    pieces = [pl.ds(0, kh)] + [pl.ds(kh + at, parted) for at in range(0, kh, parted)]
    tiles = nu // 256
    cuts = [0, tiles // 2, tiles * 4 // 5, tiles]
    for h in range(halves):
        pick(h)
        if h == 0:
            load_orb.start()
            for mu in range(mu_dev):
                load_pc(mu).start()
            pl.semaphore_wait(barrier, greetings)
        for n, cols in enumerate(pieces):
            if (n > 0) == (h > 0):
                for copy in first(cols, n):
                    copy.start()
    load_inv.wait()
    low = lax.broadcasted_iota(jnp.int32, (p, p), 0)
    high = lax.broadcasted_iota(jnp.int32, (p, p), 1)
    upper_v[...] = jnp.where(low <= high, inv_v[...].astype(F32), 0.0).astype(BF16)
    for n, cols in enumerate(pieces):
        add_rows(cols, n)
        if n == 0:
            load_orb.wait()
            turn_orbitals(cuts[0], cuts[1])
    turn_orbitals(cuts[1], cuts[2])
    for n, cols in enumerate(pieces):
        add_groups(cols, n)
        if n == 0:
            turn_orbitals(cuts[2], cuts[3])

    chunk = nu // 2
    parts = [pl.ds(i * chunk, chunk) for i in range(nu // chunk)]
    for n, cols in enumerate(pieces):
        take_rows(cols, n)

    orders = group_orders(G)
    first_mu = 0

    def make_vectors(mu):
        load_pc(mu).wait()
        left = []
        for at in parts:
            if mu is first_mu:
                correction = begun[at, :] + jnp.dot(prev_v[mu, at, kh:], rows_t[kh:, :], preferred_element_type=F32)
            else:
                correction = jnp.dot(prev_v[mu, at, :], rows_t[...], preferred_element_type=F32)
            left.append((new_v[mu, at, :].astype(F32) - correction).astype(BF16))
        for at, residual in zip(parts, left):
            new_v[mu, at, :] = jnp.dot(residual, upper_v[...], preferred_element_type=F32).astype(BF16)

    def add(slot, mu):
        here = relay_in.at[slot, mu]
        pltpu.make_async_copy(here, here, relay_sem.at[slot, mu]).wait()
        block_v[...] += relay_in[slot, mu].astype(F32)

    at_low = g == 0
    at_high = g == G - 1
    at_end = (at_low | at_high) & chained(G)

    def hop(to, at, sem):
        via = jnp.where(to > g, g + 1, g - 1)
        remote(send.at[at], relay_in.at[at], hop_sem, relay_sem.at[sem], r, via).start()

    def emit(to, mu):
        own = to == g
        if chained(G):
            from_low = jnp.logical_not(at_low) & ((to > g) | (own & at_high))
            from_high = jnp.logical_not(at_high) & ((to < g) | (own & at_low))
            pl.when(from_low | from_high)(lambda: add(to, mu))
            near = ((to == g + 1) & (to < G - 1)) | ((to == g - 1) & (to > 0))
        else:
            near = jnp.logical_not(own)

        @pl.when(own & jnp.logical_not(at_end))
        def _():
            whole = block_v[...].T
            for k in range(R):
                own_out[mu, k] = whole[k * c : (k + 1) * c, :]
            own_in[r * mu_dev + mu] = own_out[mu, r]
            for peer in everyone[:-1]:
                remote(own_out.at[mu, peer], own_in.at[r * mu_dev + mu], own_send, own_recv, peer, g).start()

        def turn_last(slot):
            turned = block_v[...].T.astype(BF16)
            for k in range(R):
                last[slot, mu, k] = turned[k * c : (k + 1) * c, :]

        @pl.when(near)
        def _():
            if chained(G):
                slot = jnp.where(to > g, 0, 1)
                into = slot
            else:
                slot = to - (to > g).astype(jnp.int32)
                into = g
            turn_last(slot)
            for peer in everyone:
                remote(
                    last.at[slot, mu, peer], last_in.at[into, r * mu_dev + mu], last_send, last_recv.at[into], peer, to
                ).start()

        if not chained(G):
            return

        @pl.when(own & at_end)
        def _():
            slot = jnp.where(at_low, 1, 0)
            turn_last(slot)
            last_in[0, r * mu_dev + mu] = last[slot, mu, r]
            for peer in everyone[:-1]:
                remote(
                    last.at[slot, mu, peer], last_in.at[0, r * mu_dev + mu], own_send, last_recv.at[0], peer, g
                ).start()

        @pl.when(jnp.logical_not(own | near))
        def _():
            send[to, mu] = block_v[...].astype(BF16)

            hop(to, (to, mu), (to, mu))

    def block(to, mu):
        at = pl.ds(pl.multiple_of(to * j_dev, j_dev), j_dev)
        block_v[...] = jnp.dot(orb_t[at, :], new_v[mu], preferred_element_type=F32)

    initial = choose(g, [order[0] for order in orders])

    make_vectors(first_mu)
    if chained(G) and G > 1:
        for half in range(2):
            rows = pl.ds(half * (j_dev // 2), j_dev // 2)
            at = pl.ds(pl.multiple_of(initial * j_dev + half * (j_dev // 2), j_dev // 2), j_dev // 2)
            block_v[rows, :] = jnp.dot(orb_t[at, :], new_v[first_mu], preferred_element_type=F32)

            @pl.when(at_end)
            def _():
                send[initial, first_mu, rows, :] = block_v[rows, :].astype(BF16)
                hop(initial, (initial, first_mu, rows), (initial, first_mu))

        pl.when(jnp.logical_not(at_end))(lambda: emit(initial, first_mu))
    else:
        block(initial, first_mu)
        emit(initial, first_mu)

    @pl.loop(1, mu_dev)
    def _(mu):
        make_vectors(mu)
        block(initial, mu)
        emit(initial, mu)

    rest = list(range(1, G))
    paired = rest[-2:] if chained(G) and G > 2 else []
    for s in rest[: len(rest) - len(paired)]:
        to = choose(g, [order[s] for order in orders])

        @pl.loop(0, mu_dev)
        def _(mu):
            block(to, mu)
            emit(to, mu)

    if paired:
        one, two = [choose(g, [order[s] for order in orders]) for s in paired]

        @pl.loop(0, 2 * mu_dev)
        def _(t):
            second_one = jnp.where(at_end, t // mu_dev, lax.rem(t, 2))
            mu = jnp.where(at_end, lax.rem(t, mu_dev), t // 2)
            to = jnp.where(second_one == 0, one, two)
            block(to, mu)
            emit(to, mu)

    def take(buf, sem, when):
        pl.when(when)(pltpu.make_async_copy(buf, buf, sem).wait)

    def gather(slot, when):
        take(last_in.at[slot], last_recv.at[slot], when)

        @pl.when(when)
        def _():
            own_in[...] += last_in[slot].astype(F32)

    def finish(slot, when):
        take(last_in.at[slot], last_recv.at[slot], when)

        @pl.when(when)
        def _():
            out_v[...] = (own_in[...] + last_in[slot].astype(F32)).astype(BF16)

    inner = jnp.logical_not(at_end)
    others = own_in.at[pl.ds(0, (R - 1) * mu_dev)]
    take(others, own_recv, inner)
    if chained(G):
        for slot, when in ((0, inner & (2 * g < G)), (1, inner & (2 * g >= G))):
            gather(1 - slot, when)
            finish(slot, when)
        rounded = last_in.at[0, pl.ds(0, (R - 1) * mu_dev)]
        take(rounded, last_recv.at[0], at_end)

        @pl.when(at_end)
        def _():
            out_v[...] = last_in[0]
    else:
        for slot in range(G):
            gather(slot, g != slot)
        out_v[...] = own_in[...].astype(BF16)

    every = pl.ds(0, k_all)
    wait_all(buf_a, R - 1, every, rows_send)
    wait_all(buf_b, G - 1, every, rows_send)
    wait_all(buf_c, R - 1, every, rows_send)
    take(others, own_send, inner)
    if chained(G):
        take(rounded, own_send, at_end)
        nears = (g + 1 < G - 1).astype(jnp.int32) + (g - 1 > 0).astype(jnp.int32)
        for count in range(3):
            if count:
                take(last.at[pl.ds(0, count)], last_send, nears == count)
            if G - 1 > count:
                take(send.at[pl.ds(0, G - 1 - count)], hop_sem, nears == count)
    else:
        take(last, last_send, inner)


def fused(pivots, columns, previous, inverse, orbitals, R, G):
    mu_dev, nu, p = columns.shape
    k = previous.shape[2]
    c = p // R
    nj = orbitals.shape[1]
    halves = 2
    kh = k // halves
    hbm = pl.BlockSpec(memory_space=pltpu.HBM)
    slots = 2 if chained(G) else G
    relays = G if chained(G) else 1
    blocks = (R * mu_dev, c, nj // G)
    vmem = pl.BlockSpec(memory_space=pltpu.VMEM)
    dma = pltpu.SemaphoreType.DMA
    return pl.pallas_call(
        functools.partial(fused_kernel, R, G),
        out_shape=(
            jax.ShapeDtypeStruct(blocks, BF16),
            jax.ShapeDtypeStruct(columns.shape, BF16),
        ),
        in_specs=[hbm, hbm, hbm, hbm, hbm],
        out_specs=(vmem, vmem),
        scratch_shapes=[
            pltpu.VMEM((1, p), jnp.int32),
            pltpu.VMEM((p, p), BF16),
            pltpu.VMEM((p, 128), jnp.int32),
            pltpu.VMEM((p, 128), BF16),
            pltpu.VMEM((mu_dev, p, nu), BF16),
            pltpu.VMEM((p, kh), F32),
            pltpu.VMEM((R, c, k), BF16),
            pltpu.VMEM((R, c, k), BF16),
            pltpu.VMEM((G, c, k), BF16),
            pltpu.VMEM((R, c, k), BF16),
            pltpu.VMEM((k, p), BF16),
            pltpu.VMEM((p, p), BF16),
            pltpu.VMEM((mu_dev, nu, k), BF16),
            pltpu.VMEM((nu, nj), BF16),
            pltpu.VMEM((nj, nu), BF16),
            pltpu.VMEM((nj // G, p), F32),
            pltpu.VMEM((nu, p), F32),
            pltpu.VMEM((relays, mu_dev, nj // G, p), BF16),
            pltpu.VMEM((relays, mu_dev, nj // G, p), BF16),
            pltpu.VMEM((2 if chained(G) else G - 1, mu_dev, R, c, nj // G), BF16),
            pltpu.VMEM((mu_dev, R, c, nj // G), F32),
            pltpu.VMEM((slots,) + blocks, BF16),
            pltpu.VMEM(blocks, F32),
            dma(()), dma((halves + 1,)), dma((halves + 1,)), dma((halves + 1,)), dma((2,)), dma((halves, mu_dev)), dma((mu_dev,)), dma(()),
            dma(()), dma((relays, mu_dev)), dma(()), dma((slots,)), dma(()), dma(()),
        ],
        compiler_params=pltpu.CompilerParams(
            collective_id=0, has_side_effects=True, vmem_limit_bytes=44 * 1024 * 1024
        ),
        name="fused_exchange",
    )(pivots, columns, previous, inverse, orbitals)


def block_kernel(part_ref, slab_ref, made_ref, out_hbm, new_hbm, out_v, part_v, spread_ref, new_sem, out_sem):
    mus, vecs, j = part_ref.shape
    groups, lot, _, _ = out_v.shape
    wide = mus * lot
    store = pltpu.make_async_copy(made_ref, new_hbm, new_sem)
    store.start()
    mu = lax.broadcasted_iota(jnp.int32, (mus, wide), 0)
    col = lax.broadcasted_iota(jnp.int32, (mus, wide), 1)
    repeat = jnp.where(lax.shift_right_logical(col, lot.bit_length() - 1) == mu, 1.0, 0.0).astype(BF16)
    spread_ref[...] = lax.dot_general(
        slab_ref[...], repeat, (((0,), (0,)), ((), ())), preferred_element_type=F32
    ).astype(BF16)
    for k in range(groups):
        part_v[k] = part_ref[:, k * lot : (k + 1) * lot, :].reshape(wide, j)

    def piece(q, k):
        return pltpu.make_async_copy(out_v.at[k, q], out_hbm.at[k, q], out_sem)

    @pl.loop(0, lot)
    def _(q):
        at = lax.broadcasted_iota(jnp.int32, spread_ref.shape, 1) & (lot - 1)
        kept = jnp.where(at == q, spread_ref[...].astype(F32), 0.0).astype(BF16)
        for k in range(groups):
            out_v[k, q] = jnp.dot(kept, part_v[k], preferred_element_type=F32).astype(BF16)
            piece(q, k).start()

    pltpu.make_async_copy(out_v, out_hbm, out_sem).wait()
    store.wait()


def orbital_block(part, slab, made):
    mus, vecs, j = part.shape
    i = slab.shape[1]
    lot = 8
    assert vecs % lot == 0
    groups = vecs // lot
    vmem = pl.BlockSpec(memory_space=pltpu.VMEM)
    anywhere = pl.BlockSpec(memory_space=pl.ANY)
    out, new = pl.pallas_call(
        block_kernel,
        out_shape=(
            jax.ShapeDtypeStruct((groups, lot, i, j), BF16),
            jax.ShapeDtypeStruct(made.shape, BF16),
        ),
        in_specs=[vmem, vmem, vmem],
        out_specs=(anywhere, anywhere),
        scratch_shapes=[
            pltpu.VMEM((groups, lot, i, j), BF16),
            pltpu.VMEM((groups, mus * lot, j), BF16),
            pltpu.VMEM((i, mus * lot), BF16),
            pltpu.SemaphoreType.DMA(()),
            pltpu.SemaphoreType.DMA(()),
        ],
        compiler_params=pltpu.CompilerParams(vmem_limit_bytes=40 * 1024 * 1024),
        name="orbital_block",
    )(part, slab, made)
    return out.reshape(vecs, i, j), new


def per_device(R, G, pivot_columns, previous, pivots, pivot_inverse, orbitals, slab_orbitals):
    count = pivot_columns.shape[2]
    stay = functools.partial(pltpu.with_memory_space_constraint, memory_space=pltpu.HBM)
    part, made = fused(
        stay(pivots.reshape(1, count)), pivot_columns, previous, stay(pivot_inverse), orbitals, R, G
    )
    mo_block, new_vectors = orbital_block(part, slab_orbitals, made)
    return new_vectors, mo_block


def solution(mesh):
    R, G = mesh.shape["rows"], mesh.shape["grp"]
    in_specs = (P("rows", "grp", None), P("rows", "grp", None), P(), P(), P("grp", None), P())
    out_specs = (P("rows", "grp", None), P("rows", None, "grp"))
    return jax.shard_map(
        functools.partial(per_device, R, G), mesh=mesh, in_specs=in_specs, out_specs=out_specs,
        check_vma=False,
    )
```

```python
import functools

import jax
import jax.numpy as jnp
from jax import lax
from jax.experimental import pallas as pl
from jax.experimental.pallas import tpu as pltpu
from jax.sharding import PartitionSpec as P

F32 = jnp.float32
BF16 = jnp.bfloat16
MESH = pl.DeviceIdType.MESH


def chained(G):
    return G <= 4


def group_orders(G):
    def due(g, d):
        if d == g:
            return 4 * G if chained(G) and g in (0, G - 1) else -1
        return 2 * (G - 1 - d) + g if d > g else 2 * d + G - 1 - g

    return [sorted(range(G), key=lambda d: (due(g, d), d)) for g in range(G)]


def choose(g, values):
    chosen = jnp.int32(values[0])
    for k in range(1, len(values)):
        chosen = jnp.where(g == k, values[k], chosen)
    return chosen


def fused_kernel(
    R, G, piv_hbm, pc_hbm, prev_hbm, inv_hbm, orb_hbm, out_v, new_v,
    piv_v, inv_v, piv_col, within, hot_v, picked, buf_x, buf_a, buf_b, buf_c, rows_t, upper_v, prev_v, orb_v, orb_t,
    block_v, begun, send, relay_in, last, own_out, last_in, own_in,
    rows_send, recv_a, recv_b, recv_c, small_sem, prev_sem, pc_sem, orb_sem,
    hop_sem, relay_sem, last_send, last_recv, own_send, own_recv,
):
    r = lax.axis_index("rows")
    g = lax.axis_index("grp")
    mu_dev, nu, p = new_v.shape
    _, _, j_dev, _ = send.shape
    _, c, k_all = buf_c.shape
    halves = 2
    kh = k_all // halves

    load_piv = pltpu.make_async_copy(piv_hbm, piv_v, small_sem.at[0])
    load_inv = pltpu.make_async_copy(inv_hbm, inv_v, small_sem.at[1])
    load_orb = pltpu.make_async_copy(orb_hbm, orb_v, orb_sem)

    def load_prev(h, mu):
        at = pl.ds(h * kh, kh)
        return pltpu.make_async_copy(prev_hbm.at[mu, :, at], prev_v.at[mu, :, at], prev_sem.at[h, mu])

    def load_pc(mu):
        return pltpu.make_async_copy(pc_hbm.at[mu], new_v.at[mu], pc_sem.at[mu])

    load_piv.start()
    barrier = pltpu.get_barrier_semaphore()

    def greet(row, grp):
        pl.semaphore_signal(barrier, inc=1, device_id={"rows": row, "grp": grp}, device_id_type=MESH)

    def greet_rows(step):
        @pl.loop(1, R)
        def _(d):
            greet(lax.rem(r + d, R), lax.rem(g + step + G, G))

    greet_rows(0)
    for d in range(1, G):
        greet(r, lax.rem(g + d, G))
    for h in range(halves):
        for mu in range(mu_dev):
            load_prev(h, mu).start()
    if chained(G):
        if G > 1:
            pl.when(g > 0)(lambda: greet_rows(-1))
            pl.when(g < G - 1)(lambda: greet_rows(1))
        sides = (g > 0).astype(jnp.int32) + (g < G - 1).astype(jnp.int32)
    else:
        for d in range(1, G):
            greet_rows(d)
        sides = G - 1
    greetings = (sides + 1) * (R - 1) + G - 1
    load_inv.start()
    load_piv.wait()

    lanes = piv_col.shape[1]
    turned_piv = jnp.broadcast_to(piv_v[...], (lanes, p)).T
    lane = lax.broadcasted_iota(jnp.int32, (p, lanes), 1)
    piv_col[...] = lax.shift_right_arithmetic(turned_piv, lanes.bit_length() - 1)
    within[...] = jnp.where((turned_piv & (lanes - 1)) == lane, 1.0, 0.0).astype(BF16)

    def heat(mu):
        base = (r * mu_dev + mu) * (nu * G) + g * nu
        tile = (piv_col[...] - base // lanes).astype(F32).astype(BF16)
        for i in range(nu // lanes):
            here = tile == jnp.full(tile.shape, i, BF16)
            hot_v[mu, :, i * lanes : (i + 1) * lanes] = jnp.where(here, within[...], jnp.zeros(tile.shape, BF16))

    def remote(src, dst, send, recv, row, grp):
        return pltpu.make_async_remote_copy(
            src_ref=src, dst_ref=dst, send_sem=send, recv_sem=recv,
            device_id={"rows": row, "grp": grp}, device_id_type=MESH,
        )

    if R & (R - 1) == 0:
        bits = [1 << b for b in range(R.bit_length() - 1)]
        flips = [(b, b - 2 * b * lax.rem(r // b, 2)) for b in bits]
        everyone = [r + sum(change for b, change in flips if m & b) for m in range(R - 1, -1, -1)]
        row_peers = [(R - 1 - k, q) for k, q in enumerate(everyone[:-1])]
    else:
        everyone = [lax.rem(r + k, R) for k in range(R - 1, -1, -1)]
        row_peers = [(R - 1 - k, q) for k, q in enumerate(everyone[:-1])]

    turns = [jnp.where(2 * g < G, G - d, d) for d in range(1, G)]
    grp_peers = [(d, lax.rem(g + d, G)) for d in turns]

    pl.loop(0, mu_dev)(heat)

    def pick(h):
        picked[...] = jnp.zeros(picked.shape, F32)

        @pl.loop(0, mu_dev)
        def _(mu):
            load_prev(h, mu).wait()
            picked[...] += jnp.dot(hot_v[mu], prev_v[mu, :, h * kh : (h + 1) * kh], preferred_element_type=F32)

        for k in range(R):
            buf_x[k, :, h * kh : (h + 1) * kh] = picked[k * c : (k + 1) * c, :].astype(BF16)

    def first(cols, n):
        return [
            remote(buf_x.at[q, :, cols], buf_a.at[d, :, cols], rows_send, recv_a.at[n], q, g) for d, q in row_peers
        ]

    def second(cols, n):
        return [
            remote(buf_b.at[0, :, cols], buf_b.at[d, :, cols], rows_send, recv_b.at[n], r, q) for d, q in grp_peers
        ]

    def third(cols, n):
        return [
            remote(buf_c.at[r, :, cols], buf_c.at[r, :, cols], rows_send, recv_c.at[n], q, g) for d, q in row_peers
        ]

    def wait_all(buf, count, cols, sem):
        if count:
            received = buf.at[pl.ds(0, count), :, cols]
            pltpu.make_async_copy(received, received, sem).wait()

    def add_rows(cols, n):
        total = buf_x[r, :, cols].astype(F32)
        wait_all(buf_a, R - 1, cols, recv_a.at[n])
        for d, _ in row_peers:
            total = total + buf_a[d, :, cols].astype(F32)
        buf_b[0, :, cols] = total.astype(BF16)
        for copy in second(cols, n):
            copy.start()

    def add_groups(cols, n):
        total = buf_b[0, :, cols].astype(F32)
        wait_all(buf_b, G - 1, cols, recv_b.at[n])
        for d, _ in grp_peers:
            total = total + buf_b[d, :, cols].astype(F32)
        buf_c[r, :, cols] = total.astype(BF16)
        for copy in third(cols, n):
            copy.start()

    def take_rows(cols, n):
        wait_all(buf_c, R - 1, cols, recv_c.at[n])
        rows_t[cols, :] = buf_c[:, :, cols].reshape(p, cols.size).astype(F32).T.astype(BF16)
        if n == 0:
            for at in parts:
                begun[at, :] = jnp.dot(prev_v[0, at, cols], rows_t[cols, :], preferred_element_type=F32)

    square = (256, 256)
    eye = jnp.where(
        lax.broadcasted_iota(jnp.int32, square, 0) == lax.broadcasted_iota(jnp.int32, square, 1), 1.0, 0.0
    ).astype(BF16)
    wide = orb_v.shape[1] // 256

    def turn_orbitals(first, last):
        @pl.loop(first, last)
        def _(i):
            at = pl.ds(pl.multiple_of(i * 256, 256), 256)
            for q in range(wide):
                orb_t[q * 256 : (q + 1) * 256, at] = lax.dot_general(
                    eye, orb_v[at, q * 256 : (q + 1) * 256], (((1,), (1,)), ((), ())), preferred_element_type=F32
                ).astype(BF16)

    parted = kh // 2 if kh % 256 == 0 else kh
    pieces = [pl.ds(0, kh)] + [pl.ds(kh + at, parted) for at in range(0, kh, parted)]
    tiles = nu // 256
    cuts = [0, tiles // 2, tiles * 7 // 10, tiles]
    for h in range(halves):
        pick(h)
        if h == 0:
            load_orb.start()
            for mu in range(mu_dev):
                load_pc(mu).start()
            pl.semaphore_wait(barrier, greetings)
        for n, cols in enumerate(pieces):
            if (n > 0) == (h > 0):
                for copy in first(cols, n):
                    copy.start()
    load_inv.wait()
    low = lax.broadcasted_iota(jnp.int32, (p, p), 0)
    high = lax.broadcasted_iota(jnp.int32, (p, p), 1)
    upper_v[...] = jnp.where(low <= high, inv_v[...].astype(F32), 0.0).astype(BF16)
    for n, cols in enumerate(pieces):
        add_rows(cols, n)
        if n == 0:
            load_orb.wait()
            turn_orbitals(cuts[0], cuts[1])
    turn_orbitals(cuts[1], cuts[2])
    for n, cols in enumerate(pieces):
        add_groups(cols, n)
        if n == 0:
            turn_orbitals(cuts[2], cuts[3])

    chunk = nu // 2
    parts = [pl.ds(i * chunk, chunk) for i in range(nu // chunk)]
    for n, cols in enumerate(pieces):
        take_rows(cols, n)

    orders = group_orders(G)
    first_mu = 0

    def make_vectors(mu):
        load_pc(mu).wait()
        left = []
        for at in parts:
            if mu is first_mu:
                correction = begun[at, :] + jnp.dot(prev_v[mu, at, kh:], rows_t[kh:, :], preferred_element_type=F32)
            else:
                correction = jnp.dot(prev_v[mu, at, :], rows_t[...], preferred_element_type=F32)
            left.append((new_v[mu, at, :].astype(F32) - correction).astype(BF16))
        for at, residual in zip(parts, left):
            new_v[mu, at, :] = jnp.dot(residual, upper_v[...], preferred_element_type=F32).astype(BF16)

    def add(slot, mu):
        here = relay_in.at[slot, mu]
        pltpu.make_async_copy(here, here, relay_sem.at[slot, mu]).wait()
        block_v[...] += relay_in[slot, mu].astype(F32)

    at_low = g == 0
    at_high = g == G - 1
    at_end = (at_low | at_high) & chained(G)

    def hop(to, at, sem):
        via = jnp.where(to > g, g + 1, g - 1)
        remote(send.at[at], relay_in.at[at], hop_sem, relay_sem.at[sem], r, via).start()

    def emit(to, mu):
        own = to == g
        if chained(G):
            from_low = jnp.logical_not(at_low) & ((to > g) | (own & at_high))
            from_high = jnp.logical_not(at_high) & ((to < g) | (own & at_low))
            pl.when(from_low | from_high)(lambda: add(to, mu))
            near = ((to == g + 1) & (to < G - 1)) | ((to == g - 1) & (to > 0))
        else:
            near = jnp.logical_not(own)

        @pl.when(own & jnp.logical_not(at_end))
        def _():
            whole = block_v[...].T
            for k in range(R):
                own_out[mu, k] = whole[k * c : (k + 1) * c, :]
            own_in[r * mu_dev + mu] = own_out[mu, r]
            for peer in everyone[:-1]:
                remote(own_out.at[mu, peer], own_in.at[r * mu_dev + mu], own_send, own_recv, peer, g).start()

        def turn_last(slot):
            turned = block_v[...].T.astype(BF16)
            for k in range(R):
                last[slot, mu, k] = turned[k * c : (k + 1) * c, :]

        @pl.when(near)
        def _():
            if chained(G):
                slot = jnp.where(to > g, 0, 1)
                into = slot
            else:
                slot = to - (to > g).astype(jnp.int32)
                into = g
            turn_last(slot)
            for peer in everyone:
                remote(
                    last.at[slot, mu, peer], last_in.at[into, r * mu_dev + mu], last_send, last_recv.at[into], peer, to
                ).start()

        if not chained(G):
            return

        @pl.when(own & at_end)
        def _():
            slot = jnp.where(at_low, 1, 0)
            turn_last(slot)
            last_in[0, r * mu_dev + mu] = last[slot, mu, r]
            for peer in everyone[:-1]:
                remote(
                    last.at[slot, mu, peer], last_in.at[0, r * mu_dev + mu], own_send, last_recv.at[0], peer, g
                ).start()

        @pl.when(jnp.logical_not(own | near))
        def _():
            send[to, mu] = block_v[...].astype(BF16)

            hop(to, (to, mu), (to, mu))

    def block(to, mu):
        at = pl.ds(pl.multiple_of(to * j_dev, j_dev), j_dev)
        block_v[...] = jnp.dot(orb_t[at, :], new_v[mu], preferred_element_type=F32)

    initial = choose(g, [order[0] for order in orders])

    make_vectors(first_mu)
    if chained(G) and G > 1:
        for half in range(2):
            rows = pl.ds(half * (j_dev // 2), j_dev // 2)
            at = pl.ds(pl.multiple_of(initial * j_dev + half * (j_dev // 2), j_dev // 2), j_dev // 2)
            block_v[rows, :] = jnp.dot(orb_t[at, :], new_v[first_mu], preferred_element_type=F32)

            @pl.when(at_end)
            def _():
                send[initial, first_mu, rows, :] = block_v[rows, :].astype(BF16)
                hop(initial, (initial, first_mu, rows), (initial, first_mu))

        pl.when(jnp.logical_not(at_end))(lambda: emit(initial, first_mu))
    else:
        block(initial, first_mu)
        emit(initial, first_mu)

    @pl.loop(1, mu_dev)
    def _(mu):
        make_vectors(mu)
        block(initial, mu)
        emit(initial, mu)

    rest = list(range(1, G))
    paired = rest[-2:] if chained(G) and G > 2 else []
    for s in rest[: len(rest) - len(paired)]:
        to = choose(g, [order[s] for order in orders])

        @pl.loop(0, mu_dev)
        def _(mu):
            block(to, mu)
            emit(to, mu)

    if paired:
        one, two = [choose(g, [order[s] for order in orders]) for s in paired]

        @pl.loop(0, 2 * mu_dev)
        def _(t):
            second_one = jnp.where(at_end, t // mu_dev, lax.rem(t, 2))
            mu = jnp.where(at_end, lax.rem(t, mu_dev), t // 2)
            to = jnp.where(second_one == 0, one, two)
            block(to, mu)
            emit(to, mu)

    def take(buf, sem, when):
        pl.when(when)(pltpu.make_async_copy(buf, buf, sem).wait)

    def gather(slot, when):
        take(last_in.at[slot], last_recv.at[slot], when)

        @pl.when(when)
        def _():
            own_in[...] += last_in[slot].astype(F32)

    def finish(slot, when):
        take(last_in.at[slot], last_recv.at[slot], when)

        @pl.when(when)
        def _():
            out_v[...] = (own_in[...] + last_in[slot].astype(F32)).astype(BF16)

    inner = jnp.logical_not(at_end)
    others = own_in.at[pl.ds(0, (R - 1) * mu_dev)]
    take(others, own_recv, inner)
    if chained(G):
        for slot, when in ((0, inner & (2 * g < G)), (1, inner & (2 * g >= G))):
            gather(1 - slot, when)
            finish(slot, when)
        rounded = last_in.at[0, pl.ds(0, (R - 1) * mu_dev)]
        take(rounded, last_recv.at[0], at_end)

        @pl.when(at_end)
        def _():
            out_v[...] = last_in[0]
    else:
        for slot in range(G):
            gather(slot, g != slot)
        out_v[...] = own_in[...].astype(BF16)

    every = pl.ds(0, k_all)
    wait_all(buf_a, R - 1, every, rows_send)
    wait_all(buf_b, G - 1, every, rows_send)
    wait_all(buf_c, R - 1, every, rows_send)
    take(others, own_send, inner)
    if chained(G):
        take(rounded, own_send, at_end)
        nears = (g + 1 < G - 1).astype(jnp.int32) + (g - 1 > 0).astype(jnp.int32)
        for count in range(3):
            if count:
                take(last.at[pl.ds(0, count)], last_send, nears == count)
            if G - 1 > count:
                take(send.at[pl.ds(0, G - 1 - count)], hop_sem, nears == count)
    else:
        take(last, last_send, inner)


def fused(pivots, columns, previous, inverse, orbitals, R, G):
    mu_dev, nu, p = columns.shape
    k = previous.shape[2]
    c = p // R
    nj = orbitals.shape[1]
    halves = 2
    kh = k // halves
    hbm = pl.BlockSpec(memory_space=pltpu.HBM)
    slots = 2 if chained(G) else G
    relays = G if chained(G) else 1
    blocks = (R * mu_dev, c, nj // G)
    vmem = pl.BlockSpec(memory_space=pltpu.VMEM)
    dma = pltpu.SemaphoreType.DMA
    return pl.pallas_call(
        functools.partial(fused_kernel, R, G),
        out_shape=(
            jax.ShapeDtypeStruct(blocks, BF16),
            jax.ShapeDtypeStruct(columns.shape, BF16),
        ),
        in_specs=[hbm, hbm, hbm, hbm, hbm],
        out_specs=(vmem, vmem),
        scratch_shapes=[
            pltpu.VMEM((1, p), jnp.int32),
            pltpu.VMEM((p, p), BF16),
            pltpu.VMEM((p, 128), jnp.int32),
            pltpu.VMEM((p, 128), BF16),
            pltpu.VMEM((mu_dev, p, nu), BF16),
            pltpu.VMEM((p, kh), F32),
            pltpu.VMEM((R, c, k), BF16),
            pltpu.VMEM((R, c, k), BF16),
            pltpu.VMEM((G, c, k), BF16),
            pltpu.VMEM((R, c, k), BF16),
            pltpu.VMEM((k, p), BF16),
            pltpu.VMEM((p, p), BF16),
            pltpu.VMEM((mu_dev, nu, k), BF16),
            pltpu.VMEM((nu, nj), BF16),
            pltpu.VMEM((nj, nu), BF16),
            pltpu.VMEM((nj // G, p), F32),
            pltpu.VMEM((nu, p), F32),
            pltpu.VMEM((relays, mu_dev, nj // G, p), BF16),
            pltpu.VMEM((relays, mu_dev, nj // G, p), BF16),
            pltpu.VMEM((2 if chained(G) else G - 1, mu_dev, R, c, nj // G), BF16),
            pltpu.VMEM((mu_dev, R, c, nj // G), F32),
            pltpu.VMEM((slots,) + blocks, BF16),
            pltpu.VMEM(blocks, F32),
            dma(()), dma((halves + 1,)), dma((halves + 1,)), dma((halves + 1,)), dma((2,)), dma((halves, mu_dev)), dma((mu_dev,)), dma(()),
            dma(()), dma((relays, mu_dev)), dma(()), dma((slots,)), dma(()), dma(()),
        ],
        compiler_params=pltpu.CompilerParams(
            collective_id=0, has_side_effects=True, vmem_limit_bytes=44 * 1024 * 1024
        ),
        name="fused_exchange",
    )(pivots, columns, previous, inverse, orbitals)


def block_kernel(part_ref, slab_ref, made_ref, out_hbm, new_hbm, out_v, part_v, spread_ref, new_sem, out_sem):
    mus, vecs, j = part_ref.shape
    groups, lot, _, _ = out_v.shape
    wide = mus * lot
    store = pltpu.make_async_copy(made_ref, new_hbm, new_sem)
    store.start()
    mu = lax.broadcasted_iota(jnp.int32, (mus, wide), 0)
    col = lax.broadcasted_iota(jnp.int32, (mus, wide), 1)
    repeat = jnp.where(lax.shift_right_logical(col, lot.bit_length() - 1) == mu, 1.0, 0.0).astype(BF16)
    spread_ref[...] = lax.dot_general(
        slab_ref[...], repeat, (((0,), (0,)), ((), ())), preferred_element_type=F32
    ).astype(BF16)
    for k in range(groups):
        part_v[k] = part_ref[:, k * lot : (k + 1) * lot, :].reshape(wide, j)

    def piece(q, k):
        return pltpu.make_async_copy(out_v.at[k, q], out_hbm.at[k, q], out_sem)

    @pl.loop(0, lot)
    def _(q):
        at = lax.broadcasted_iota(jnp.int32, spread_ref.shape, 1) & (lot - 1)
        kept = jnp.where(at == q, spread_ref[...].astype(F32), 0.0).astype(BF16)
        for k in range(groups):
            out_v[k, q] = jnp.dot(kept, part_v[k], preferred_element_type=F32).astype(BF16)
            piece(q, k).start()

    pltpu.make_async_copy(out_v, out_hbm, out_sem).wait()
    store.wait()


def orbital_block(part, slab, made):
    mus, vecs, j = part.shape
    i = slab.shape[1]
    lot = 8
    assert vecs % lot == 0
    groups = vecs // lot
    vmem = pl.BlockSpec(memory_space=pltpu.VMEM)
    anywhere = pl.BlockSpec(memory_space=pl.ANY)
    out, new = pl.pallas_call(
        block_kernel,
        out_shape=(
            jax.ShapeDtypeStruct((groups, lot, i, j), BF16),
            jax.ShapeDtypeStruct(made.shape, BF16),
        ),
        in_specs=[vmem, vmem, vmem],
        out_specs=(anywhere, anywhere),
        scratch_shapes=[
            pltpu.VMEM((groups, lot, i, j), BF16),
            pltpu.VMEM((groups, mus * lot, j), BF16),
            pltpu.VMEM((i, mus * lot), BF16),
            pltpu.SemaphoreType.DMA(()),
            pltpu.SemaphoreType.DMA(()),
        ],
        compiler_params=pltpu.CompilerParams(vmem_limit_bytes=40 * 1024 * 1024),
        name="orbital_block",
    )(part, slab, made)
    return out.reshape(vecs, i, j), new


def per_device(R, G, pivot_columns, previous, pivots, pivot_inverse, orbitals, slab_orbitals):
    count = pivot_columns.shape[2]
    stay = functools.partial(pltpu.with_memory_space_constraint, memory_space=pltpu.HBM)
    part, made = fused(
        stay(pivots.reshape(1, count)), pivot_columns, previous, stay(pivot_inverse), orbitals, R, G
    )
    mo_block, new_vectors = orbital_block(part, slab_orbitals, made)
    return new_vectors, mo_block


def solution(mesh):
    R, G = mesh.shape["rows"], mesh.shape["grp"]
    in_specs = (P("rows", "grp", None), P("rows", "grp", None), P(), P(), P("grp", None), P())
    out_specs = (P("rows", "grp", None), P("rows", None, "grp"))
    return jax.shard_map(
        functools.partial(per_device, R, G), mesh=mesh, in_specs=in_specs, out_specs=out_specs,
        check_vma=False,
    )
```
